32 devices in a mesh: grp: 4 (over x, core), mem: 8 (over z, y).
Axes of the slice: x: 2, y: 2, z: 4, core: 2. Of those that a mesh axis runs over, the one named last changes fastest.
Arguments:
- child_field: float32 [2, 1024, 4096], P(None, None, ('grp', 'mem')), may hold values from -6 to 6
- theta_interp: float32 [64, 32], replicated, may hold values from -1 to 1
- phi_interp: float32 [64, 32], replicated, may hold values from -1 to 1
- child_phase: float32 [8, 4096], replicated, may hold values from -3.140625 to 3.140625
- translation: float32 [2, 316, 4096], P(None, None, 'mem'), may hold values from -0.3125 to 0.3125
- inter_source: int32 [32, 24], P('grp'), may hold values from 0 to 31, as said below
- inter_kind: int32 [32, 24], P('grp'), may hold values from 0 to 315
- inter_count: int32 [32], P('grp'), may hold values from 6 to 24
Outputs:
- child_out: float32 [2, 1024, 4096], P(None, None, ('grp', 'mem'))
The draws below stay inside these ranges and needn't reach their ends.
Inputs may be any that keep to these rules, and one draw needn't show every extreme that they name: The source box of every slot lies in its target's group of 8 consecutive parent boxes or in one of the two groups beside it: inter_source[t, k] // 8 differs from t // 8 by at most one. Slots from inter_count[t] on are unused.
All inputs are finite; a program needn't handle non-finite values.
Results may differ from the reference program's by a relative error of at most 0.0003.
Values sent between devices are 32-bit elements; how exact they have to be, the bound alone decides.
No kernel may reach another device: no remote copies, remote signals or barrier semaphores. Data moves between devices by JAX's collectives and lax.ppermute only.
A program may use at most 64 MiB of HBM per device.

```python
import jax
import jax.numpy as jnp
from jax import lax

L1T = 32
L1P = 32
L2T = 64
L2P = 64
SAMPLES1 = 1024
SAMPLES2 = 4096
WAVES = 16
BRANCH = 8
SLOTS = 24
NTRANS = 316
GROUPS = 4
GROUP_PARENTS = 8
PARENTS = 32
CHILDREN = 256


def draw_inter_source(key, part):
    first_key, second_key = jax.random.split(jax.random.fold_in(key, 11))
    target_group = (jnp.arange(PARENTS, dtype=jnp.int32) // GROUP_PARENTS)[:, None]
    stepping = jax.random.randint(first_key, (PARENTS, SLOTS), -1, 2)
    source_group = jnp.clip(target_group + stepping, 0, GROUPS - 1)
    member_pick = jax.random.randint(second_key, (PARENTS, SLOTS), 0, GROUP_PARENTS)
    return (source_group * GROUP_PARENTS + member_pick).astype(jnp.int32)


def plant(entries, own_key, smallest, largest):
    longest = entries.shape.index(max(entries.shape))
    spots = []
    for shift in (0, 1):
        where = [jax.random.randint(jax.random.fold_in(own_key, axis), (), 0, length) for axis, length in enumerate(entries.shape)]
        where[longest] = (where[longest] + shift) % entries.shape[longest]
        spots.append(tuple(where))
    return entries.at[spots[0]].set(smallest).at[spots[1]].set(largest)


def level_of(own_key, extent, cuts, low, largest):
    gain = 1.0
    for axis_at, blocks in cuts:
        steps = jax.random.uniform(jax.random.fold_in(jax.random.fold_in(own_key, 6), axis_at), (blocks,), jnp.float32, low / len(cuts), largest / len(cuts))
        gain = gain * jnp.repeat(jnp.exp(steps), extent[axis_at] // blocks).reshape((-1,) + (1,) * (len(extent) - 1 - axis_at))
    return gain


def normal_values(stream_key, dims, width, bound, cuts=(), held_as=jnp.bfloat16):
    array = width * jax.random.normal(stream_key, dims, jnp.float32)
    if cuts:
        array = array * level_of(stream_key, dims, cuts, -0.22, 0.18)
    return jnp.clip(array, -bound, bound).astype(held_as)


def setup_inputs(seed: int = 0) -> dict:
    key_of = jax.random.split(jax.random.key(seed), 9)
    return {
        "child_field": normal_values(key_of[0], (2, SAMPLES1, CHILDREN * WAVES), 1.0, 6.0, ((2, 32),), jnp.float32),
        "theta_interp": normal_values(key_of[1], (L2T, L1T), L1T ** -0.5, 1.0, (), jnp.float32),
        "phi_interp": normal_values(key_of[2], (L2P, L1P), L1P ** -0.5, 1.0, (), jnp.float32),
        "child_phase": jnp.clip(jax.random.uniform(key_of[3], (BRANCH, SAMPLES2), jnp.float32, -3.140625, 3.140625), -3.140625, 3.140625),
        "translation": normal_values(key_of[4], (2, NTRANS, SAMPLES2), (16 * SLOTS) ** -0.5, 0.3125, ((2, 8),), jnp.float32),
        "inter_source": draw_inter_source(jax.random.fold_in(key_of[8], 71), 0),
        "inter_kind": plant(jax.random.randint(key_of[6], (PARENTS, SLOTS), 0, NTRANS), jax.random.fold_in(key_of[6], 1), 0, NTRANS - 1).astype(jnp.int32),
        "inter_count": plant(jax.random.randint(key_of[7], (PARENTS,), SLOTS // 4, SLOTS + 1), jax.random.fold_in(key_of[7], 1), SLOTS // 4, SLOTS).astype(jnp.int32),
    }


precise = lax.Precision.HIGHEST


def spread_out(samples, theta_interp, phi_interp):
    columns = samples.shape[2]
    arranged = samples.reshape(2, theta_interp.shape[1], phi_interp.shape[1], columns)
    middle = jnp.einsum("at,ctpr->capr", theta_interp, arranged, precision=precise)
    fine_grid = jnp.einsum("bp,capr->cabr", phi_interp, middle, precision=precise)
    return fine_grid.reshape(2, theta_interp.shape[0] * phi_interp.shape[0], columns)


def fold_back(samples, theta_interp, phi_interp):
    columns = samples.shape[2]
    arranged = samples.reshape(2, theta_interp.shape[0], phi_interp.shape[0], columns)
    middle = jnp.einsum("bp,cabr->capr", phi_interp, arranged, precision=precise)
    coarse = jnp.einsum("at,capr->ctpr", theta_interp, middle, precision=precise)
    return coarse.reshape(2, theta_interp.shape[1] * phi_interp.shape[1], columns)


def reference(child_field, theta_interp, phi_interp, child_phase, translation, inter_source, inter_kind, inter_count):
    branch = child_phase.shape[0]
    cosine = jnp.cos(child_phase).T[:, :, None]
    sine_table = jnp.sin(child_phase).T[:, :, None]
    block_width = branch * WAVES
    parent_ids = jnp.arange(PARENTS, dtype=jnp.int32)

    def gather_parent(parent):
        child_block = lax.dynamic_slice_in_dim(child_field, parent * block_width, block_width, 2)
        fine_grid = spread_out(child_block, theta_interp, phi_interp)
        grouped = fine_grid.reshape(2, fine_grid.shape[1], branch, WAVES)
        real_part = grouped[0] * cosine - grouped[1] * sine_table
        imag_part = grouped[1] * cosine + grouped[0] * sine_table
        return jnp.stack([jnp.sum(real_part, axis=1), jnp.sum(imag_part, axis=1)])

    outgoing = lax.map(gather_parent, parent_ids)
    slot_index = jnp.arange(SLOTS, dtype=jnp.int32)

    def translate_one(pieces):
        sources, kind_rows, live_count = pieces
        weight = (slot_index < live_count).astype(jnp.float32)
        picked = jnp.take(outgoing, sources, axis=0)
        factor = jnp.take(translation, kind_rows, axis=1) * weight[None, :, None]
        real_part = jnp.sum(factor[0][:, :, None] * picked[:, 0] - factor[1][:, :, None] * picked[:, 1], axis=0)
        imag_part = jnp.sum(factor[0][:, :, None] * picked[:, 1] + factor[1][:, :, None] * picked[:, 0], axis=0)
        return jnp.stack([real_part, imag_part])

    incoming = lax.map(translate_one, (inter_source, inter_kind, inter_count))

    def scatter_parent(parent):
        parent_field = incoming[parent]
        real_part = parent_field[0][:, None, :] * cosine + parent_field[1][:, None, :] * sine_table
        imag_part = parent_field[1][:, None, :] * cosine - parent_field[0][:, None, :] * sine_table
        local_field = jnp.stack([real_part, imag_part]).reshape(2, parent_field.shape[1], block_width)
        return fold_back(local_field, theta_interp, phi_interp)

    blocks = lax.map(scatter_parent, parent_ids)
    return jnp.transpose(blocks, (1, 2, 0, 3)).reshape(2, SAMPLES1, PARENTS * block_width)
```

```python
import functools

import jax
import jax.numpy as jnp
from jax import lax
from jax.experimental import pallas as pl
from jax.experimental.pallas import tpu as pltpu
from jax.sharding import PartitionSpec as P

f32 = jnp.float32
bf16 = jnp.bfloat16
SUB = 8
BLOCK = 256
UNROLL = 4


def split(x):
    hi = x.astype(bf16)
    lo = (x - hi.astype(f32)).astype(bf16)
    return hi, lo


def mm(a, b):
    return jnp.dot(a, b, preferred_element_type=f32)


def mm_tn(a, b):
    return lax.dot_general(a, b, (((0,), (0,)), ((), ())), preferred_element_type=f32)


def iota(shape, dim):
    return lax.broadcasted_iota(jnp.int32, shape, dim)


def picker(shape, test):
    return jnp.where(test(iota(shape, 0), iota(shape, 1)), 1.0, 0.0).astype(bf16)


def sincos(q):
    r = q * 0.5
    z = r * r
    s = 1.0 / 6227020800.0
    for c in (-1.0 / 39916800.0, 1.0 / 362880.0, -1.0 / 5040.0, 1.0 / 120.0, -1.0 / 6.0, 1.0):
        s = s * z + c
    s = s * r
    k = 1.0 / 479001600.0
    for c in (-1.0 / 3628800.0, 1.0 / 40320.0, -1.0 / 720.0, 1.0 / 24.0, -0.5, 1.0):
        k = k * z + c
    return 2.0 * s * k, 1.0 - 2.0 * s * s


def aggregate_kernel(x_ref, theta_ref, phi_ref, phase_ref, o_ref, mid_ref, cos_ref, sin_ref):
    coarse_t, fine_t = theta_ref.shape
    coarse_p, fine_p = phi_ref.shape
    groups = coarse_p // SUB
    span = BLOCK // fine_p
    per_member = o_ref.shape[3]
    waves = o_ref.shape[2]
    branch = phase_ref.shape[0]
    columns = branch * waves

    spread_t = picker((coarse_t, coarse_t * SUB), lambda r, c: r == c // SUB)
    big = (fine_t * SUB, coarse_t * SUB)
    keep = iota(big, 0) % SUB == iota(big, 1) % SUB

    def theta_block(part):
        rows = mm_tn(part, spread_t)
        rows = jnp.broadcast_to(rows[:, None, :], (fine_t, SUB, coarse_t * SUB)).reshape(big)
        return jnp.where(keep, rows, 0.0).astype(bf16)

    th, tl = split(theta_ref[...])
    kh, kl = theta_block(th), theta_block(tl)
    weights = jnp.concatenate([kh, kh, kl], axis=1)

    spread_p = picker((fine_p, BLOCK), lambda r, c: r == c % fine_p)
    small = (span * coarse_p, BLOCK)
    diag = iota(small, 0) // coarse_p == iota(small, 1) // fine_p

    def phi_block(part):
        rows = mm(part, spread_p)
        rows = jnp.concatenate([rows] * span, axis=0)
        return jnp.where(diag, rows, 0.0).astype(bf16)

    ph, pl_ = split(phi_ref[...])
    bh, bl = phi_block(ph), phi_block(pl_)
    phi_weights = jnp.concatenate([bh, bh, bl], axis=0)

    sine, cosine = sincos(phase_ref[...])
    cos_ref[...] = cosine
    sin_ref[...] = sine

    for g in range(groups):
        parts = [x_ref[c, :, g].reshape(coarse_t * SUB, columns) for c in range(2)]
        hi, lo = split(jnp.concatenate(parts, axis=1))
        middle = mm(weights, jnp.concatenate([hi, lo, hi], axis=0))
        mid_ref[:, g] = middle.reshape(fine_t, SUB, 2 * columns)

    unit = min(BLOCK, per_member)

    def body(step, carry):
        start = step * BLOCK
        rows = mid_ref[pl.ds(step * span, span)].reshape(span * coarse_p, 2 * columns)
        hi, lo = split(rows.T)
        fine = mm(jnp.concatenate([hi, lo, hi], axis=1), phi_weights)
        real = fine[:columns].reshape(branch, waves, BLOCK)
        imag = fine[columns:].reshape(branch, waves, BLOCK)
        lanes = pl.ds(pl.multiple_of(start, BLOCK), BLOCK)
        c = cos_ref[:, lanes][:, None, :]
        s = sin_ref[:, lanes][:, None, :]
        out_real = jnp.sum(real * c - imag * s, axis=0)
        out_imag = jnp.sum(imag * c + real * s, axis=0)
        for piece in range(BLOCK // unit):
            at = start + piece * unit
            member = at // per_member
            offset = pl.multiple_of(at - member * per_member, unit)
            here = slice(piece * unit, (piece + 1) * unit)
            o_ref[member, 0, :, pl.ds(offset, unit)] = out_real[:, here]
            o_ref[member, 1, :, pl.ds(offset, unit)] = out_imag[:, here]
        return carry

    lax.fori_loop(0, fine_t // span, body, 0)


def translate_kernel(source_ref, kind_ref, count_ref, base_ref, factor_ref, own_ref, before_ref, after_ref, o_ref, all_ref, sems):
    members = own_ref.shape[0]
    targets, slots = source_ref.shape
    copies = [
        pltpu.make_async_copy(ref, all_ref.at[pl.ds(i * members, members)], sems.at[i])
        for i, ref in enumerate((before_ref, own_ref, after_ref))
    ]
    for copy in copies:
        copy.start()
    for copy in copies:
        copy.wait()
    base = base_ref[0]
    waves, directions = o_ref.shape[2:]

    def target_body(t, carry):
        count = count_ref[t]

        def slot_body(step, acc):
            real, imag = acc
            for i in range(UNROLL):
                k = step * UNROLL + i
                live = k < count
                at = jnp.where(live, source_ref[t, k] - base, 0)
                kind = jnp.where(live, kind_ref[t, k], 0)
                weight = jnp.where(live, 1.0, 0.0).astype(f32)
                factor = factor_ref[kind] * weight
                fr = factor[0:1]
                fi = factor[1:2]
                sr = all_ref[at, 0]
                si = all_ref[at, 1]
                real = real + (fr * sr - fi * si)
                imag = imag + (fr * si + fi * sr)
            return real, imag

        zero = jnp.zeros((waves, directions), f32)
        real, imag = lax.fori_loop(0, (count + UNROLL - 1) // UNROLL, slot_body, (zero, zero))
        o_ref[t, 0] = real
        o_ref[t, 1] = imag
        return carry

    lax.fori_loop(0, targets, target_body, 0)


def disaggregate_kernel(r_ref, theta_ref, phi_ref, phase_ref, o_ref, mid_ref, cos_ref, sin_ref):
    coarse_t, fine_t = theta_ref.shape
    coarse_p, fine_p = phi_ref.shape
    groups = coarse_p // SUB
    span = BLOCK // fine_p
    per_member = r_ref.shape[3]
    waves = r_ref.shape[2]
    branch = phase_ref.shape[0]
    columns = branch * waves

    spread_t = picker((fine_t, fine_t * SUB), lambda r, c: r == c // SUB)
    big = (coarse_t * SUB, fine_t * SUB)
    keep = iota(big, 0) % SUB == iota(big, 1) % SUB

    def theta_block(part):
        rows = mm(part, spread_t)
        rows = jnp.broadcast_to(rows[:, None, :], (coarse_t, SUB, fine_t * SUB)).reshape(big)
        return jnp.where(keep, rows, 0.0).astype(bf16)

    th, tl = split(theta_ref[...])
    kh, kl = theta_block(th), theta_block(tl)
    weights = jnp.concatenate([kh, kh, kl], axis=1)

    narrow = span * coarse_p
    spread_p = picker((coarse_p, narrow), lambda r, c: r == c % coarse_p)
    small = (BLOCK, narrow)
    diag = iota(small, 0) // fine_p == iota(small, 1) // coarse_p

    def phi_block(part):
        rows = mm_tn(part, spread_p)
        rows = jnp.concatenate([rows] * span, axis=0)
        return jnp.where(diag, rows, 0.0).astype(bf16)

    ph, pl_ = split(phi_ref[...])
    phi_weights = jnp.concatenate([phi_block(ph), phi_block(pl_)], axis=1)

    sine, cosine = sincos(phase_ref[...])
    cos_ref[...] = cosine
    sin_ref[...] = sine
    unit = min(BLOCK, per_member)

    def body(step, carry):
        start = step * BLOCK
        pieces = []
        for piece in range(BLOCK // unit):
            at = start + piece * unit
            member = at // per_member
            offset = pl.multiple_of(at - member * per_member, unit)
            pieces.append([r_ref[member, c, :, pl.ds(offset, unit)] for c in range(2)])
        real = jnp.concatenate([p[0] for p in pieces], axis=1)[None]
        imag = jnp.concatenate([p[1] for p in pieces], axis=1)[None]
        lanes = pl.ds(pl.multiple_of(start, BLOCK), BLOCK)
        c = cos_ref[:, lanes][:, None, :]
        s = sin_ref[:, lanes][:, None, :]
        local = jnp.concatenate(
            [
                (real * c + imag * s).reshape(columns, BLOCK),
                (imag * c - real * s).reshape(columns, BLOCK),
            ],
            axis=0,
        )
        hi, lo = split(local)
        y = mm(jnp.concatenate([hi, lo], axis=0), phi_weights)
        rows = 2 * columns
        folded = y[:rows, :narrow] + (y[rows:, :narrow] + y[:rows, narrow:])
        mid_ref[pl.ds(step * span, span)] = folded.T.reshape(span, groups, SUB, rows)
        return carry

    lax.fori_loop(0, fine_t // span, body, 0)

    for g in range(groups):
        hi, lo = split(mid_ref[:, g].reshape(fine_t * SUB, 2 * columns))
        coarse = mm(weights, jnp.concatenate([hi, lo, hi], axis=0))
        o_ref[0, :, g] = coarse[:, :columns].reshape(coarse_t, SUB, columns)
        o_ref[1, :, g] = coarse[:, columns:].reshape(coarse_t, SUB, columns)


def vmem():
    return pl.BlockSpec(memory_space=pltpu.VMEM)


def smem():
    return pl.BlockSpec(memory_space=pltpu.SMEM)


def hbm():
    return pl.BlockSpec(memory_space=pltpu.HBM)


def per_device(
    child_field,
    theta_interp,
    phi_interp,
    child_phase,
    translation,
    inter_source,
    inter_kind,
    inter_count,
    *,
    interpret=False,
):
    call = functools.partial(pl.pallas_call, interpret=interpret)
    branch, fine = child_phase.shape
    columns = child_field.shape[2]
    waves = columns // branch
    fine_t, coarse_t = theta_interp.shape
    fine_p, coarse_p = phi_interp.shape
    groups = coarse_p // SUB
    members = lax.axis_size("mem")
    grp_count = lax.axis_size("grp")
    per_member = fine // members
    theta_t = theta_interp.T
    phi_t = phi_interp.T
    scratch = [
        pltpu.VMEM((fine_t, groups, SUB, 2 * columns), f32),
        pltpu.VMEM((branch, fine), f32),
        pltpu.VMEM((branch, fine), f32),
    ]
    block = jax.ShapeDtypeStruct((members, 2, waves, per_member), f32)
    summed = call(
        aggregate_kernel,
        out_shape=block,
        in_specs=[vmem()] * 4,
        out_specs=vmem(),
        scratch_shapes=scratch,
    )(child_field.reshape(2, coarse_t, groups, SUB, columns), theta_t, phi_t, child_phase)

    own = lax.all_to_all(summed, "mem", split_axis=0, concat_axis=0, tiled=True)
    up = [(i, i + 1) for i in range(grp_count - 1)]
    before = lax.ppermute(own, "grp", up)
    after = lax.ppermute(own, "grp", [(j, i) for i, j in up])
    base = ((lax.axis_index("grp") - 1) * members).astype(jnp.int32).reshape(1)

    incoming = call(
        translate_kernel,
        out_shape=block,
        in_specs=[smem()] * 4 + [vmem()] + [hbm()] * 3,
        out_specs=vmem(),
        scratch_shapes=[
            pltpu.VMEM((3 * members, 2, waves, per_member), f32),
            pltpu.SemaphoreType.DMA((3,)),
        ],
    )(inter_source, inter_kind, inter_count, base, jnp.transpose(translation, (1, 0, 2)), own, before, after)

    returned = lax.all_to_all(incoming, "mem", split_axis=0, concat_axis=0, tiled=True)
    out = call(
        disaggregate_kernel,
        out_shape=jax.ShapeDtypeStruct((2, coarse_t, groups, SUB, columns), f32),
        in_specs=[vmem()] * 4,
        out_specs=vmem(),
        scratch_shapes=scratch,
    )(returned, theta_t, phi_t, child_phase)
    return out.reshape(child_field.shape)


def solution(mesh):
    return jax.shard_map(
        per_device,
        mesh=mesh,
        in_specs=(
            P(None, None, ("grp", "mem")),
            P(),
            P(),
            P(),
            P(None, None, "mem"),
            P("grp", None),
            P("grp", None),
            P("grp"),
        ),
        out_specs=P(None, None, ("grp", "mem")),
        check_vma=False,
    )
```

```python
import functools

import jax
import jax.numpy as jnp
from jax import lax
from jax.experimental import pallas as pl
from jax.experimental.pallas import tpu as pltpu
from jax.sharding import PartitionSpec as P

f32 = jnp.float32
bf16 = jnp.bfloat16
SUB = 8
BLOCK = 256
UNROLL = 4
COST = 50_000_000
VMEM_LIMIT = 20 << 20


def split(x):
    hi = x.astype(bf16)
    lo = (x - hi.astype(f32)).astype(bf16)
    return hi, lo


def mm(a, b):
    return jnp.dot(a, b, preferred_element_type=f32)


def mm_tn(a, b):
    return lax.dot_general(a, b, (((0,), (0,)), ((), ())), preferred_element_type=f32)


def iota(shape, dim):
    return lax.broadcasted_iota(jnp.int32, shape, dim)


def picker(shape, test):
    return jnp.where(test(iota(shape, 0), iota(shape, 1)), 1.0, 0.0).astype(bf16)


def sincos(q):
    r = q * 0.5
    z = r * r
    s = 1.0 / 6227020800.0
    for c in (-1.0 / 39916800.0, 1.0 / 362880.0, -1.0 / 5040.0, 1.0 / 120.0, -1.0 / 6.0, 1.0):
        s = s * z + c
    s = s * r
    k = 1.0 / 479001600.0
    for c in (-1.0 / 3628800.0, 1.0 / 40320.0, -1.0 / 720.0, 1.0 / 24.0, -0.5, 1.0):
        k = k * z + c
    return 2.0 * s * k, 1.0 - 2.0 * s * s


def plan(fine, members):
    per_member = fine // members
    chunks = max(1, per_member // BLOCK)
    return chunks, fine // BLOCK // chunks


def aggregate_kernel(x_ref, theta_ref, phi_ref, phase_ref, o_ref, mid_ref, cos_ref, sin_ref, *, chunk, chunks):
    coarse_t, fine_t = theta_ref.shape
    coarse_p, fine_p = phi_ref.shape
    groups = coarse_p // SUB
    span = BLOCK // fine_p
    per_member = o_ref.shape[3]
    waves = o_ref.shape[2]
    branch = phase_ref.shape[0]
    columns = branch * waves
    kept = fine_t // chunks

    chosen = picker((fine_t, kept), lambda r, c: r == (c // span * chunks + chunk) * span + c % span)
    spread_t = picker((coarse_t, coarse_t * SUB), lambda r, c: r == c // SUB)
    big = (kept * SUB, coarse_t * SUB)
    keep = iota(big, 0) % SUB == iota(big, 1) % SUB

    def theta_block(part):
        rows = mm_tn(mm(part, chosen).astype(bf16), spread_t)
        rows = jnp.broadcast_to(rows[:, None, :], (kept, SUB, coarse_t * SUB)).reshape(big)
        return jnp.where(keep, rows, 0.0).astype(bf16)

    th, tl = split(theta_ref[...])
    kh, kl = theta_block(th), theta_block(tl)
    weights = jnp.concatenate([kh, kh, kl], axis=1)

    spread_p = picker((fine_p, BLOCK), lambda r, c: r == c % fine_p)
    small = (span * coarse_p, BLOCK)
    diag = iota(small, 0) // coarse_p == iota(small, 1) // fine_p

    def phi_block(part):
        rows = mm(part, spread_p)
        rows = jnp.concatenate([rows] * span, axis=0)
        return jnp.where(diag, rows, 0.0).astype(bf16)

    ph, pl_ = split(phi_ref[...])
    bh, bl = phi_block(ph), phi_block(pl_)
    phi_weights = jnp.concatenate([bh, bh, bl], axis=0)

    sine, cosine = sincos(phase_ref[...])
    cos_ref[...] = cosine
    sin_ref[...] = sine

    for g in range(groups):
        parts = [x_ref[c, :, g].reshape(coarse_t * SUB, columns) for c in range(2)]
        hi, lo = split(jnp.concatenate(parts, axis=1))
        middle = mm(weights, jnp.concatenate([hi, lo, hi], axis=0))
        mid_ref[:, g] = middle.reshape(kept, SUB, 2 * columns)

    unit = min(BLOCK, per_member)

    def body(step, carry):
        rows = mid_ref[pl.ds(step * span, span)].reshape(span * coarse_p, 2 * columns)
        hi, lo = split(rows.T)
        fine = mm(jnp.concatenate([hi, lo, hi], axis=1), phi_weights)
        real = fine[:columns].reshape(branch, waves, BLOCK)
        imag = fine[columns:].reshape(branch, waves, BLOCK)
        lanes = pl.ds(pl.multiple_of((step * chunks + chunk) * BLOCK, BLOCK), BLOCK)
        c = cos_ref[:, lanes][:, None, :]
        s = sin_ref[:, lanes][:, None, :]
        out_real = jnp.sum(real * c - imag * s, axis=0)
        out_imag = jnp.sum(imag * c + real * s, axis=0)
        for piece in range(BLOCK // unit):
            here = slice(piece * unit, (piece + 1) * unit)
            member = step * (BLOCK // unit) + piece
            o_ref[member, 0] = out_real[:, here]
            o_ref[member, 1] = out_imag[:, here]
        return carry

    lax.fori_loop(0, kept // span, body, 0)


def translate_kernel(source_ref, kind_ref, count_ref, base_ref, factor_ref, own_ref, before_ref, after_ref, o_ref, all_ref, *, chunk):
    members = own_ref.shape[0]
    targets, slots = source_ref.shape
    for i, ref in enumerate((before_ref, own_ref, after_ref)):
        all_ref[pl.ds(i * members, members)] = ref[...]
    base = base_ref[0]
    waves, directions = o_ref.shape[2:]
    lanes = pl.ds(chunk * directions, directions)

    def target_body(t, carry):
        count = count_ref[t]

        def slot_body(step, acc):
            real, imag = acc
            for i in range(UNROLL):
                k = step * UNROLL + i
                live = k < count
                at = jnp.where(live, source_ref[t, k] - base, 0)
                kind = jnp.where(live, kind_ref[t, k], 0)
                weight = jnp.where(live, 1.0, 0.0).astype(f32)
                factor = factor_ref[kind, :, lanes] * weight
                fr = factor[0:1]
                fi = factor[1:2]
                sr = all_ref[at, 0]
                si = all_ref[at, 1]
                real = real + (fr * sr - fi * si)
                imag = imag + (fr * si + fi * sr)
            return real, imag

        zero = jnp.zeros((waves, directions), f32)
        real, imag = lax.fori_loop(0, (count + UNROLL - 1) // UNROLL, slot_body, (zero, zero))
        o_ref[t, 0] = real
        o_ref[t, 1] = imag
        return carry

    lax.fori_loop(0, targets, target_body, 0)


def disaggregate_kernel(*refs, chunk, chunks, first):
    if first:
        r_ref, theta_ref, phi_ref, phase_ref, o_ref, mid_ref, cos_ref, sin_ref = refs
    else:
        r_ref, theta_ref, phi_ref, phase_ref, partial_ref, o_ref, mid_ref, cos_ref, sin_ref = refs
    coarse_t, fine_t = theta_ref.shape
    coarse_p, fine_p = phi_ref.shape
    groups = coarse_p // SUB
    span = BLOCK // fine_p
    per_member = r_ref.shape[3]
    waves = r_ref.shape[2]
    branch = phase_ref.shape[0]
    columns = branch * waves
    kept = fine_t // chunks

    def source_row(c):
        a = c // SUB
        return (a // span * chunks + chunk) * span + a % span

    spread_t = picker((fine_t, kept * SUB), lambda r, c: r == source_row(c))
    big = (coarse_t * SUB, kept * SUB)
    keep = iota(big, 0) % SUB == iota(big, 1) % SUB

    def theta_block(part):
        rows = mm(part, spread_t)
        rows = jnp.broadcast_to(rows[:, None, :], (coarse_t, SUB, kept * SUB)).reshape(big)
        return jnp.where(keep, rows, 0.0).astype(bf16)

    th, tl = split(theta_ref[...])
    kh, kl = theta_block(th), theta_block(tl)
    weights = jnp.concatenate([kh, kh, kl], axis=1)

    narrow = span * coarse_p
    spread_p = picker((coarse_p, narrow), lambda r, c: r == c % coarse_p)
    small = (BLOCK, narrow)
    diag = iota(small, 0) // fine_p == iota(small, 1) // coarse_p

    def phi_block(part):
        rows = mm_tn(part, spread_p)
        rows = jnp.concatenate([rows] * span, axis=0)
        return jnp.where(diag, rows, 0.0).astype(bf16)

    ph, pl_ = split(phi_ref[...])
    phi_weights = jnp.concatenate([phi_block(ph), phi_block(pl_)], axis=1)

    sine, cosine = sincos(phase_ref[...])
    cos_ref[...] = cosine
    sin_ref[...] = sine
    unit = min(BLOCK, per_member)

    def body(step, carry):
        many = BLOCK // unit
        parts = [[r_ref[step * many + piece, c] for piece in range(many)] for c in range(2)]
        real, imag = [jnp.concatenate(p, axis=1)[None] for p in parts]
        lanes = pl.ds(pl.multiple_of((step * chunks + chunk) * BLOCK, BLOCK), BLOCK)
        c = cos_ref[:, lanes][:, None, :]
        s = sin_ref[:, lanes][:, None, :]
        local = jnp.concatenate(
            [
                (real * c + imag * s).reshape(columns, BLOCK),
                (imag * c - real * s).reshape(columns, BLOCK),
            ],
            axis=0,
        )
        hi, lo = split(local)
        y = mm(jnp.concatenate([hi, lo], axis=0), phi_weights)
        rows = 2 * columns
        folded = y[:rows, :narrow] + (y[rows:, :narrow] + y[:rows, narrow:])
        mid_ref[pl.ds(step * span, span)] = folded.T.reshape(span, groups, SUB, rows)
        return carry

    lax.fori_loop(0, kept // span, body, 0)

    for g in range(groups):
        hi, lo = split(mid_ref[:, g].reshape(kept * SUB, 2 * columns))
        coarse = mm(weights, jnp.concatenate([hi, lo, hi], axis=0))
        for c in range(2):
            part = coarse[:, c * columns : (c + 1) * columns].reshape(coarse_t, SUB, columns)
            o_ref[c, :, g] = part if first else part + partial_ref[c, :, g]


def vmem():
    return pl.BlockSpec(memory_space=pltpu.VMEM)


def smem():
    return pl.BlockSpec(memory_space=pltpu.SMEM)


def per_device(
    child_field,
    theta_interp,
    phi_interp,
    child_phase,
    translation,
    inter_source,
    inter_kind,
    inter_count,
    *,
    interpret=False,
):
    call = functools.partial(
        pl.pallas_call,
        interpret=interpret,
        out_specs=vmem(),
        compiler_params=pltpu.CompilerParams(vmem_limit_bytes=VMEM_LIMIT),
    )
    branch, fine = child_phase.shape
    columns = child_field.shape[2]
    waves = columns // branch
    fine_t, coarse_t = theta_interp.shape
    coarse_p = phi_interp.shape[1]
    groups = coarse_p // SUB
    members = lax.axis_size("mem")
    grp_count = lax.axis_size("grp")
    chunks, steps = plan(fine, members)
    width = fine // members // chunks
    theta_t = theta_interp.T
    phi_t = phi_interp.T
    factors = jnp.transpose(translation, (1, 0, 2))
    scratch = [
        pltpu.VMEM((fine_t // chunks, groups, SUB, 2 * columns), f32),
        pltpu.VMEM((branch, fine), f32),
        pltpu.VMEM((branch, fine), f32),
    ]
    block = jax.ShapeDtypeStruct((members, 2, waves, width), f32)
    field = child_field.reshape(2, coarse_t, groups, SUB, columns)
    base = ((lax.axis_index("grp") - 1) * members).astype(jnp.int32).reshape(1)
    up = [(i, i + 1) for i in range(grp_count - 1)]
    down = [(j, i) for i, j in up]

    def exchange(x):
        return lax.all_to_all(x, "mem", split_axis=0, concat_axis=0, tiled=True)

    received = []
    for h in range(chunks):
        summed = call(
            functools.partial(aggregate_kernel, chunk=h, chunks=chunks),
            out_shape=block,
            in_specs=[vmem()] * 4,
            scratch_shapes=scratch,
            name=f"aggregate{h}",
            cost_estimate=pl.CostEstimate(flops=COST, transcendentals=0, bytes_accessed=1 << 20),
        )(field, theta_t, phi_t, child_phase)
        received.append(exchange(summed))
    returned = []
    for h in range(chunks):
        own = received[h]
        incoming = call(
            functools.partial(translate_kernel, chunk=h),
            out_shape=block,
            in_specs=[smem()] * 4 + [vmem()] * 4,
            scratch_shapes=[pltpu.VMEM((3 * members, 2, waves, width), f32)],
            name=f"translate{h}",
            cost_estimate=pl.CostEstimate(flops=COST, transcendentals=0, bytes_accessed=1 << 20),
        )(inter_source, inter_kind, inter_count, base, factors, own, lax.ppermute(own, "grp", up), lax.ppermute(own, "grp", down))
        returned.append(exchange(incoming))
    out = None
    for h in range(chunks):
        first = h == 0
        out = call(
            functools.partial(disaggregate_kernel, chunk=h, chunks=chunks, first=first),
            out_shape=jax.ShapeDtypeStruct(field.shape, f32),
            in_specs=[vmem()] * (4 if first else 5),
            scratch_shapes=scratch,
            name=f"disaggregate{h}",
            cost_estimate=pl.CostEstimate(flops=COST, transcendentals=0, bytes_accessed=1 << 20),
        )(*((returned[h], theta_t, phi_t, child_phase) + (() if first else (out,))))
    return out.reshape(child_field.shape)


def solution(mesh):
    return jax.shard_map(
        per_device,
        mesh=mesh,
        in_specs=(
            P(None, None, ("grp", "mem")),
            P(),
            P(),
            P(),
            P(None, None, "mem"),
            P("grp", None),
            P("grp", None),
            P("grp"),
        ),
        out_specs=P(None, None, ("grp", "mem")),
        check_vma=False,
    )
```

```python
import jax
import jax.numpy as jnp
from jax import lax
from jax.experimental import pallas as pl
from jax.experimental.pallas import tpu as pltpu
from jax.sharding import PartitionSpec as P

f32 = jnp.float32
bf16 = jnp.bfloat16
SUB = 8
BLOCK = 256
UNROLL = 4
PAIR = 2
COST = 50_000_000
VMEM_LIMIT = 20 << 20
VMEM_WHOLE = 60 * 1024 * 1024


def split(x):
    hi = x.astype(bf16)
    lo = (x - hi.astype(f32)).astype(bf16)
    return hi, lo


def mm(a, b):
    return jnp.dot(a, b, preferred_element_type=f32)


def mm_tn(a, b):
    return lax.dot_general(a, b, (((0,), (0,)), ((), ())), preferred_element_type=f32)


def iota(shape, dim):
    return lax.broadcasted_iota(jnp.int32, shape, dim)


def picker(shape, test):
    return jnp.where(test(iota(shape, 0), iota(shape, 1)), 1.0, 0.0).astype(bf16)


def sincos(q):
    r = q * 0.5
    z = r * r
    s = 1.0 / 6227020800.0
    for c in (-1.0 / 39916800.0, 1.0 / 362880.0, -1.0 / 5040.0, 1.0 / 120.0, -1.0 / 6.0, 1.0):
        s = s * z + c
    s = s * r
    k = 1.0 / 479001600.0
    for c in (-1.0 / 3628800.0, 1.0 / 40320.0, -1.0 / 720.0, 1.0 / 24.0, -0.5, 1.0):
        k = k * z + c
    return 2.0 * s * k, 1.0 - 2.0 * s * s


def theta_rows(part, count, spread, keep):
    rows = spread(part)
    wide = rows.shape[1]
    rows = jnp.broadcast_to(rows[:, None, :], (count, SUB, wide)).reshape(count * SUB, wide)
    return jnp.where(keep, rows, 0.0).astype(bf16)


def aggregate_kernel(x_ref, theta_ref, phi_ref, phase_ref, o_ref, x_buf, theta_buf, phi_buf, phase_buf, o_buf, mid_ref, cos_ref, sin_ref, x_sems, sems, o_sems):
    coarse_t, fine_t = theta_ref.shape
    coarse_p, fine_p = phi_ref.shape
    groups = coarse_p // SUB
    span = BLOCK // fine_p
    members, _, waves, per_member = o_ref.shape
    branch, fine = phase_ref.shape
    columns = branch * waves

    small = [
        pltpu.make_async_copy(a, b, sems.at[i])
        for i, (a, b) in enumerate(((theta_ref, theta_buf), (phi_ref, phi_buf), (phase_ref, phase_buf)))
    ]
    large = [pltpu.make_async_copy(x_ref.at[:, :, g], x_buf.at[:, :, g], x_sems.at[g]) for g in range(groups)]
    for copy in small + large:
        copy.start()
    for copy in small:
        copy.wait()

    spread_t = picker((coarse_t, coarse_t * SUB), lambda r, c: r == c // SUB)
    big = (fine_t * SUB, coarse_t * SUB)
    keep = iota(big, 0) % SUB == iota(big, 1) % SUB
    kh, kl = [theta_rows(part, fine_t, lambda p: mm_tn(p, spread_t), keep) for part in split(theta_buf[...])]
    weights = jnp.concatenate([kh, kh, kl], axis=1)

    spread_p = picker((fine_p, BLOCK), lambda r, c: r == c % fine_p)
    shape = (span * coarse_p, BLOCK)
    diag = iota(shape, 0) // coarse_p == iota(shape, 1) // fine_p

    def phi_block(part):
        rows = jnp.concatenate([mm(part, spread_p)] * span, axis=0)
        return jnp.where(diag, rows, 0.0).astype(bf16)

    bh, bl = [phi_block(part) for part in split(phi_buf[...])]
    phi_weights = jnp.concatenate([bh, bh, bl], axis=0)

    sine, cosine = sincos(phase_buf[...])
    cos_ref[...] = cosine
    sin_ref[...] = sine

    for g in range(groups):
        large[g].wait()
        parts = [x_buf[c, :, g].reshape(coarse_t * SUB, columns) for c in range(2)]
        hi, lo = split(jnp.concatenate(parts, axis=1))
        middle = mm(weights, jnp.concatenate([hi, lo, hi], axis=0))
        mid_ref[:, g] = middle.reshape(fine_t, SUB, 2 * columns)

    unit = min(BLOCK, per_member)
    batch = max(per_member, PAIR * BLOCK)
    many = batch // per_member

    def out_copy(member):
        return pltpu.make_async_copy(o_buf.at[member], o_ref.at[member], o_sems.at[member])

    def body(step, carry):
        for i in range(batch // BLOCK):
            rows = mid_ref[pl.ds((step * (batch // BLOCK) + i) * span, span)].reshape(span * coarse_p, 2 * columns)
            hi, lo = split(rows.T)
            fine_part = mm(jnp.concatenate([hi, lo, hi], axis=1), phi_weights)
            real = fine_part[:columns].reshape(branch, waves, BLOCK)
            imag = fine_part[columns:].reshape(branch, waves, BLOCK)
            lanes = pl.ds(pl.multiple_of(step * batch + i * BLOCK, BLOCK), BLOCK)
            c = cos_ref[:, lanes][:, None, :]
            s = sin_ref[:, lanes][:, None, :]
            outs = jnp.sum(real * c - imag * s, axis=0), jnp.sum(imag * c + real * s, axis=0)
            for piece in range(BLOCK // unit):
                at = i * BLOCK + piece * unit
                member = step * many + at // per_member
                there = pl.ds(at % per_member, unit)
                for part in range(2):
                    o_buf[member, part, :, there] = outs[part][:, piece * unit : (piece + 1) * unit]
        for j in range(many):
            out_copy(step * many + j).start()
        return carry

    lax.fori_loop(0, fine // batch, body, 0)

    def drain(member, carry):
        out_copy(member).wait()
        return carry

    lax.fori_loop(0, members, drain, 0)


def add_slots(entry_of, count, factor_ref, data_ref, acc, wide):
    def slot_body(step, acc):
        real, imag = acc
        for i in range(UNROLL):
            k = step * UNROLL + i
            live = k < count
            entry = jnp.where(live, entry_of(k), 0)
            kind = lax.div(entry, wide)
            at = entry - kind * wide
            factor = factor_ref[kind] * jnp.where(live, 1.0, 0.0).astype(f32)
            fr = factor[0:1]
            fi = factor[1:2]
            sr = data_ref[at, 0]
            si = data_ref[at, 1]
            real = real + (fr * sr - fi * si)
            imag = imag + (fr * si + fi * sr)
        return real, imag

    return lax.fori_loop(0, lax.div(count + (UNROLL - 1), UNROLL), slot_body, acc)


def near_kernel(source_ref, kind_ref, count_ref, group_ref, factor_ref, own_ref, twin_ref, theta_ref, phi_ref, phase_ref, o_ref, far_ref, far_count_ref, theta_out, phi_out, cos_ref, sin_ref, list_ref, near_count_ref, all_ref):
    members = own_ref.shape[0]
    targets, slots = source_ref.shape
    waves, directions = o_ref.shape[2:]
    wide = 2 * members
    group = group_ref[0]
    far_group = group + 2 * (group & 1) - 1

    def sort_target(t, carry):
        count = count_ref[t]

        def sort_slot(k, counts):
            near, far = counts
            source = source_ref[t, k]
            place = lax.div(source, members)
            at = source - place * members
            entry = kind_ref[t, k] * wide + at
            list_ref[t, near] = entry + jnp.where(place == group, 0, members)
            far_ref[t, far] = entry
            is_far = jnp.where(place == far_group, 1, 0)
            return near + 1 - is_far, far + is_far

        near, far = lax.fori_loop(0, count, sort_slot, (0, 0))
        near_count_ref[t] = near
        far_count_ref[t] = far
        return carry

    lax.fori_loop(0, targets, sort_target, 0)

    all_ref[pl.ds(0, members)] = own_ref[...]
    all_ref[pl.ds(members, members)] = twin_ref[...]

    def target_body(t, carry):
        zero = jnp.zeros((waves, directions), f32)
        real, imag = add_slots(lambda k: list_ref[t, k], near_count_ref[t], factor_ref, all_ref, (zero, zero), wide)
        o_ref[t, 0] = real
        o_ref[t, 1] = imag
        return carry

    lax.fori_loop(0, targets, target_body, 0)

    coarse_t, fine_t = theta_ref.shape
    coarse_p, fine_p = phi_ref.shape
    span = BLOCK // fine_p
    spread_t = picker((fine_t, fine_t * SUB), lambda r, c: r == c // SUB)
    big = (coarse_t * SUB, fine_t * SUB)
    keep = iota(big, 0) % SUB == iota(big, 1) % SUB
    kh, kl = [theta_rows(part, coarse_t, lambda p: mm(p, spread_t), keep) for part in split(theta_ref[...])]
    theta_out[...] = jnp.concatenate([kh, kh, kl], axis=1)
    narrow = span * coarse_p
    spread_p = picker((coarse_p, narrow), lambda r, c: r == c % coarse_p)
    shape = (BLOCK, narrow)
    diag = iota(shape, 0) // fine_p == iota(shape, 1) // coarse_p

    def phi_block(part):
        rows = jnp.concatenate([mm_tn(part, spread_p)] * span, axis=0)
        return jnp.where(diag, rows, 0.0).astype(bf16)

    phi_out[...] = jnp.concatenate([phi_block(part) for part in split(phi_ref[...])], axis=1)
    sine, cosine = sincos(phase_ref[...])
    cos_ref[...] = cosine
    sin_ref[...] = sine


def far_kernel(far_ref, far_count_ref, factor_ref, data_ref, near_ref, o_ref):
    targets = near_ref.shape[0]
    wide = 2 * data_ref.shape[0]

    def target_body(t, carry):
        acc = near_ref[t, 0], near_ref[t, 1]
        real, imag = add_slots(lambda k: far_ref[t, k], far_count_ref[t], factor_ref, data_ref, acc, wide)
        o_ref[t, 0] = real
        o_ref[t, 1] = imag
        return carry

    lax.fori_loop(0, targets, target_body, 0)


def disaggregate_kernel(r_ref, weights_ref, phi_weights_ref, cos_ref, sin_ref, o_ref, o_buf, mid_ref, sems):
    fine_t, groups, _, rows = mid_ref.shape
    narrow = phi_weights_ref.shape[1] // 2
    span = narrow // (groups * SUB)
    per_member = r_ref.shape[3]
    columns = rows // 2
    coarse_t = o_ref.shape[1]
    unit = min(BLOCK, per_member)
    many = BLOCK // unit

    def body(pair, carry):
        for i in range(PAIR):
            step = pair * PAIR + i
            parts = [[], []]
            for piece in range(many):
                at = step * BLOCK + piece * unit
                member = lax.div(at, per_member)
                offset = pl.multiple_of(at - member * per_member, unit)
                for part in range(2):
                    parts[part].append(r_ref[member, part, :, pl.ds(offset, unit)])
            real, imag = [jnp.concatenate(p, axis=1)[None] for p in parts]
            lanes = pl.ds(pl.multiple_of(step * BLOCK, BLOCK), BLOCK)
            c = cos_ref[:, lanes][:, None, :]
            s = sin_ref[:, lanes][:, None, :]
            local = jnp.concatenate(
                [
                    (real * c + imag * s).reshape(columns, BLOCK),
                    (imag * c - real * s).reshape(columns, BLOCK),
                ],
                axis=0,
            )
            hi, lo = split(local)
            y = mm(jnp.concatenate([hi, lo], axis=0), phi_weights_ref[...])
            folded = y[:rows, :narrow] + (y[rows:, :narrow] + y[:rows, narrow:])
            mid_ref[pl.ds(step * span, span)] = folded.T.reshape(span, groups, SUB, rows)
        return carry

    lax.fori_loop(0, fine_t // span // PAIR, body, 0)

    copies = []
    for g in range(groups):
        hi, lo = split(mid_ref[:, g].reshape(fine_t * SUB, rows))
        coarse = mm(weights_ref[...], jnp.concatenate([hi, lo, hi], axis=0))
        for part in range(2):
            o_buf[part, :, g] = coarse[:, part * columns : (part + 1) * columns].reshape(coarse_t, SUB, columns)
        copies.append(pltpu.make_async_copy(o_buf.at[:, :, g], o_ref.at[:, :, g], sems.at[g]))
        copies[-1].start()
    for copy in copies:
        copy.wait()


def vmem():
    return pl.BlockSpec(memory_space=pltpu.VMEM)


def smem():
    return pl.BlockSpec(memory_space=pltpu.SMEM)


def hbm():
    return pl.BlockSpec(memory_space=pltpu.HBM)


def per_device(
    child_field,
    theta_interp,
    phi_interp,
    child_phase,
    translation,
    inter_source,
    inter_kind,
    inter_count,
    *,
    interpret=False,
):
    def call(*args, limit=VMEM_LIMIT, **kw):
        params = pltpu.CompilerParams(vmem_limit_bytes=limit)
        return pl.pallas_call(*args, interpret=interpret, compiler_params=params, **kw)

    shape = jax.ShapeDtypeStruct
    dma = pltpu.SemaphoreType.DMA
    branch, fine = child_phase.shape
    columns = child_field.shape[2]
    waves = columns // branch
    fine_t, coarse_t = theta_interp.shape
    fine_p, coarse_p = phi_interp.shape
    groups = coarse_p // SUB
    narrow = BLOCK // fine_p * coarse_p
    members = lax.axis_size("mem")
    grp_count = lax.axis_size("grp")
    per_member = fine // members
    targets, slots = inter_source.shape
    theta_t = theta_interp.T
    phi_t = phi_interp.T
    factors = jnp.transpose(translation, (1, 0, 2))
    block = (members, 2, waves, per_member)
    field = child_field.reshape(2, coarse_t, groups, SUB, columns)
    mid = pltpu.VMEM((fine_t, groups, SUB, 2 * columns), f32)
    phases = (branch, fine)

    summed = call(
        aggregate_kernel,
        out_shape=shape(block, f32),
        in_specs=[hbm()] * 4,
        out_specs=hbm(),
        scratch_shapes=[
            pltpu.VMEM(field.shape, f32),
            pltpu.VMEM(theta_t.shape, f32),
            pltpu.VMEM(phi_t.shape, f32),
            pltpu.VMEM(phases, f32),
            pltpu.VMEM(block, f32),
            mid,
            pltpu.VMEM(phases, f32),
            pltpu.VMEM(phases, f32),
            dma((groups,)),
            dma((3,)),
            dma((members,)),
        ],
        name="aggregate",
        limit=VMEM_WHOLE,
    )(field, theta_t, phi_t, child_phase)

    def exchange(x):
        return lax.all_to_all(x, "mem", split_axis=0, concat_axis=0, tiled=True)

    def swap(x, first):
        pairs = [(i, i + 1) for i in range(first, grp_count - 1, 2)]
        return lax.ppermute(x, "grp", pairs + [(j, i) for i, j in pairs])

    own = exchange(summed)
    far = swap(own, 1)
    twin = swap(own, 0)
    group = lax.axis_index("grp").astype(jnp.int32).reshape(1)
    near_cost = pl.CostEstimate(flops=COST, transcendentals=0, bytes_accessed=1 << 20)
    partial, far_list, far_count, theta_w, phi_w, cosine, sine = call(
        near_kernel,
        out_shape=(
            shape(block, f32),
            shape((targets, slots + 1), jnp.int32),
            shape((targets,), jnp.int32),
            shape((coarse_t * SUB, 3 * fine_t * SUB), bf16),
            shape((BLOCK, 2 * narrow), bf16),
            shape(phases, f32),
            shape(phases, f32),
        ),
        in_specs=[smem()] * 4 + [vmem()] * 6,
        out_specs=(vmem(), smem(), smem(), vmem(), vmem(), vmem(), vmem()),
        scratch_shapes=[
            pltpu.SMEM((targets, slots + 1), jnp.int32),
            pltpu.SMEM((targets,), jnp.int32),
            pltpu.VMEM((2 * members,) + block[1:], f32),
        ],
        name="near",
        cost_estimate=near_cost,
    )(inter_source, inter_kind, inter_count, group, factors, own, twin, theta_t, phi_t, child_phase)

    incoming = call(
        far_kernel,
        out_shape=shape(block, f32),
        in_specs=[smem()] * 2 + [vmem()] * 3,
        out_specs=vmem(),
        name="far",
    )(far_list, far_count, factors, far, partial)

    out = call(
        disaggregate_kernel,
        out_shape=shape(field.shape, f32),
        in_specs=[vmem()] * 5,
        out_specs=hbm(),
        scratch_shapes=[pltpu.VMEM(field.shape, f32), mid, dma((groups,))],
        name="disaggregate",
    )(exchange(incoming), theta_w, phi_w, cosine, sine)
    return out.reshape(child_field.shape)


def solution(mesh):
    return jax.shard_map(
        per_device,
        mesh=mesh,
        in_specs=(
            P(None, None, ("grp", "mem")),
            P(),
            P(),
            P(),
            P(None, None, "mem"),
            P("grp", None),
            P("grp", None),
            P("grp"),
        ),
        out_specs=P(None, None, ("grp", "mem")),
        check_vma=False,
    )
```

```python
import jax
import jax.numpy as jnp
from jax import lax
from jax.experimental import pallas as pl
from jax.experimental.pallas import tpu as pltpu
from jax.sharding import PartitionSpec as P

f32 = jnp.float32
bf16 = jnp.bfloat16
SUB = 8
BLOCK = 256
UNROLL = 4
PAIR = 16
COST = 50_000_000
VMEM_LIMIT = 20 << 20
VMEM_WHOLE = 60 * 1024 * 1024


def split(x):
    hi = x.astype(bf16)
    lo = (x - hi.astype(f32)).astype(bf16)
    return hi, lo


def mm(a, b):
    return jnp.dot(a, b, preferred_element_type=f32)


def mm_tn(a, b):
    return lax.dot_general(a, b, (((0,), (0,)), ((), ())), preferred_element_type=f32)


def iota(shape, dim):
    return lax.broadcasted_iota(jnp.int32, shape, dim)


def picker(shape, test):
    return jnp.where(test(iota(shape, 0), iota(shape, 1)), 1.0, 0.0).astype(bf16)


def sincos(q):
    r = q * 0.5
    z = r * r
    s = 1.0 / 6227020800.0
    for c in (-1.0 / 39916800.0, 1.0 / 362880.0, -1.0 / 5040.0, 1.0 / 120.0, -1.0 / 6.0, 1.0):
        s = s * z + c
    s = s * r
    k = 1.0 / 479001600.0
    for c in (-1.0 / 3628800.0, 1.0 / 40320.0, -1.0 / 720.0, 1.0 / 24.0, -0.5, 1.0):
        k = k * z + c
    return 2.0 * s * k, 1.0 - 2.0 * s * s


def theta_rows(part, count, spread, keep):
    rows = spread(part)
    wide = rows.shape[1]
    rows = jnp.broadcast_to(rows[:, None, :], (count, SUB, wide)).reshape(count * SUB, wide)
    return jnp.where(keep, rows, 0.0).astype(bf16)


def aggregate_kernel(x_ref, theta_ref, phi_ref, phase_ref, o_ref, x_buf, theta_buf, phi_buf, phase_buf, mid_ref, cos_ref, sin_ref, x_sems, sems):
    coarse_t, fine_t = theta_ref.shape
    coarse_p, fine_p = phi_ref.shape
    groups = coarse_p // SUB
    span = BLOCK // fine_p
    members, _, waves, per_member = o_ref.shape
    branch, fine = phase_ref.shape
    columns = branch * waves

    small = [
        pltpu.make_async_copy(a, b, sems.at[i])
        for i, (a, b) in enumerate(((theta_ref, theta_buf), (phi_ref, phi_buf), (phase_ref, phase_buf)))
    ]
    large = [pltpu.make_async_copy(x_ref.at[:, :, g], x_buf.at[:, :, g], x_sems.at[g]) for g in range(groups)]
    for copy in small + large:
        copy.start()
    for copy in small:
        copy.wait()

    spread_t = picker((coarse_t, coarse_t * SUB), lambda r, c: r == c // SUB)
    big = (fine_t * SUB, coarse_t * SUB)
    keep = iota(big, 0) % SUB == iota(big, 1) % SUB
    kh, kl = [theta_rows(part, fine_t, lambda p: mm_tn(p, spread_t), keep) for part in split(theta_buf[...])]
    weights = jnp.concatenate([kh, kh, kl], axis=1)

    spread_p = picker((fine_p, BLOCK), lambda r, c: r == c % fine_p)
    shape = (span * coarse_p, BLOCK)
    diag = iota(shape, 0) // coarse_p == iota(shape, 1) // fine_p

    def phi_block(part):
        rows = jnp.concatenate([mm(part, spread_p)] * span, axis=0)
        return jnp.where(diag, rows, 0.0).astype(bf16)

    bh, bl = [phi_block(part) for part in split(phi_buf[...])]
    phi_weights = jnp.concatenate([bh, bh, bl], axis=0)

    sine, cosine = sincos(phase_buf[...])
    cos_ref[...] = cosine
    sin_ref[...] = sine

    for g in range(groups):
        large[g].wait()
        parts = [x_buf[c, :, g].reshape(coarse_t * SUB, columns) for c in range(2)]
        hi, lo = split(jnp.concatenate(parts, axis=1))
        middle = mm(weights, jnp.concatenate([hi, lo, hi], axis=0))
        mid_ref[:, g] = middle.reshape(fine_t, SUB, 2 * columns)

    unit = min(BLOCK, per_member)
    batch = max(per_member, PAIR * BLOCK)
    many = batch // per_member

    def body(step, carry):
        for i in range(batch // BLOCK):
            rows = mid_ref[pl.ds((step * (batch // BLOCK) + i) * span, span)].reshape(span * coarse_p, 2 * columns)
            hi, lo = split(rows.T)
            fine_part = mm(jnp.concatenate([hi, lo, hi], axis=1), phi_weights)
            real = fine_part[:columns].reshape(branch, waves, BLOCK)
            imag = fine_part[columns:].reshape(branch, waves, BLOCK)
            lanes = pl.ds(pl.multiple_of(step * batch + i * BLOCK, BLOCK), BLOCK)
            c = cos_ref[:, lanes][:, None, :]
            s = sin_ref[:, lanes][:, None, :]
            outs = jnp.sum(real * c - imag * s, axis=0), jnp.sum(imag * c + real * s, axis=0)
            for piece in range(BLOCK // unit):
                at = i * BLOCK + piece * unit
                member = step * many + at // per_member
                there = pl.ds(at % per_member, unit)
                for part in range(2):
                    o_ref[member, part, :, there] = outs[part][:, piece * unit : (piece + 1) * unit]
        return carry

    lax.fori_loop(0, fine // batch, body, 0)


def add_slots(entry_of, count, factor_ref, data_ref, acc, wide):
    def slot_body(step, acc):
        real, imag = acc
        for i in range(UNROLL):
            k = step * UNROLL + i
            live = k < count
            entry = jnp.where(live, entry_of(k), 0)
            kind = lax.div(entry, wide)
            at = entry - kind * wide
            factor = factor_ref[kind] * jnp.where(live, 1.0, 0.0).astype(f32)
            fr = factor[0:1]
            fi = factor[1:2]
            sr = data_ref[at, 0]
            si = data_ref[at, 1]
            real = real + (fr * sr - fi * si)
            imag = imag + (fr * si + fi * sr)
        return real, imag

    return lax.fori_loop(0, lax.div(count + (UNROLL - 1), UNROLL), slot_body, acc)


def near_kernel(source_ref, kind_ref, count_ref, group_ref, factor_ref, own_ref, twin_ref, theta_ref, phi_ref, phase_ref, o_ref, far_ref, far_count_ref, theta_out, phi_out, cos_ref, sin_ref, list_ref, near_count_ref, all_ref):
    members = own_ref.shape[0]
    targets, slots = source_ref.shape
    waves, directions = o_ref.shape[2:]
    wide = 2 * members
    group = group_ref[0]
    far_group = group + 2 * (group & 1) - 1

    def sort_target(t, carry):
        count = count_ref[t]

        def sort_slot(k, counts):
            near, far = counts
            source = source_ref[t, k]
            place = lax.div(source, members)
            at = source - place * members
            entry = kind_ref[t, k] * wide + at
            list_ref[t, near] = entry + jnp.where(place == group, 0, members)
            far_ref[t, far] = entry
            is_far = jnp.where(place == far_group, 1, 0)
            return near + 1 - is_far, far + is_far

        near, far = lax.fori_loop(0, count, sort_slot, (0, 0))
        near_count_ref[t] = near
        far_count_ref[t] = far
        return carry

    lax.fori_loop(0, targets, sort_target, 0)

    all_ref[pl.ds(0, members)] = own_ref[...]
    all_ref[pl.ds(members, members)] = twin_ref[...]

    def target_body(t, carry):
        zero = jnp.zeros((waves, directions), f32)
        real, imag = add_slots(lambda k: list_ref[t, k], near_count_ref[t], factor_ref, all_ref, (zero, zero), wide)
        o_ref[t, 0] = real
        o_ref[t, 1] = imag
        return carry

    lax.fori_loop(0, targets, target_body, 0)

    coarse_t, fine_t = theta_ref.shape
    coarse_p, fine_p = phi_ref.shape
    span = BLOCK // fine_p
    spread_t = picker((fine_t, fine_t * SUB), lambda r, c: r == c // SUB)
    big = (coarse_t * SUB, fine_t * SUB)
    keep = iota(big, 0) % SUB == iota(big, 1) % SUB
    kh, kl = [theta_rows(part, coarse_t, lambda p: mm(p, spread_t), keep) for part in split(theta_ref[...])]
    theta_out[...] = jnp.concatenate([kh, kh, kl], axis=1)
    narrow = span * coarse_p
    spread_p = picker((coarse_p, narrow), lambda r, c: r == c % coarse_p)
    shape = (BLOCK, narrow)
    diag = iota(shape, 0) // fine_p == iota(shape, 1) // coarse_p

    def phi_block(part):
        rows = jnp.concatenate([mm_tn(part, spread_p)] * span, axis=0)
        return jnp.where(diag, rows, 0.0).astype(bf16)

    phi_out[...] = jnp.concatenate([phi_block(part) for part in split(phi_ref[...])], axis=1)
    sine, cosine = sincos(phase_ref[...])
    cos_ref[...] = cosine
    sin_ref[...] = sine


def far_kernel(far_ref, far_count_ref, factor_ref, data_ref, near_ref, o_ref):
    targets = near_ref.shape[0]
    wide = 2 * data_ref.shape[0]

    def target_body(t, carry):
        acc = near_ref[t, 0], near_ref[t, 1]
        real, imag = add_slots(lambda k: far_ref[t, k], far_count_ref[t], factor_ref, data_ref, acc, wide)
        o_ref[t, 0] = real
        o_ref[t, 1] = imag
        return carry

    lax.fori_loop(0, targets, target_body, 0)


def disaggregate_kernel(r_ref, weights_ref, phi_weights_ref, cos_ref, sin_ref, o_ref, o_buf, mid_ref, sems):
    fine_t, groups, _, rows = mid_ref.shape
    narrow = phi_weights_ref.shape[1] // 2
    span = narrow // (groups * SUB)
    per_member = r_ref.shape[3]
    columns = rows // 2
    coarse_t = o_ref.shape[1]
    unit = min(BLOCK, per_member)
    many = BLOCK // unit

    def body(pair, carry):
        for i in range(PAIR):
            step = pair * PAIR + i
            parts = [[], []]
            for piece in range(many):
                at = step * BLOCK + piece * unit
                member = lax.div(at, per_member)
                offset = pl.multiple_of(at - member * per_member, unit)
                for part in range(2):
                    parts[part].append(r_ref[member, part, :, pl.ds(offset, unit)])
            real, imag = [jnp.concatenate(p, axis=1)[None] for p in parts]
            lanes = pl.ds(pl.multiple_of(step * BLOCK, BLOCK), BLOCK)
            c = cos_ref[:, lanes][:, None, :]
            s = sin_ref[:, lanes][:, None, :]
            local = jnp.concatenate(
                [
                    (real * c + imag * s).reshape(columns, BLOCK),
                    (imag * c - real * s).reshape(columns, BLOCK),
                ],
                axis=0,
            )
            hi, lo = split(local)
            y = mm(jnp.concatenate([hi, lo], axis=0), phi_weights_ref[...])
            folded = y[:rows, :narrow] + (y[rows:, :narrow] + y[:rows, narrow:])
            mid_ref[pl.ds(step * span, span)] = folded.T.reshape(span, groups, SUB, rows)
        return carry

    lax.fori_loop(0, fine_t // span // PAIR, body, 0)

    copies = []
    for g in range(groups):
        hi, lo = split(mid_ref[:, g].reshape(fine_t * SUB, rows))
        coarse = mm(weights_ref[...], jnp.concatenate([hi, lo, hi], axis=0))
        for part in range(2):
            o_buf[part, :, g] = coarse[:, part * columns : (part + 1) * columns].reshape(coarse_t, SUB, columns)
        copies.append(pltpu.make_async_copy(o_buf.at[:, :, g], o_ref.at[:, :, g], sems.at[g]))
        copies[-1].start()
    for copy in copies:
        copy.wait()


def vmem():
    return pl.BlockSpec(memory_space=pltpu.VMEM)


def smem():
    return pl.BlockSpec(memory_space=pltpu.SMEM)


def hbm():
    return pl.BlockSpec(memory_space=pltpu.HBM)


def per_device(
    child_field,
    theta_interp,
    phi_interp,
    child_phase,
    translation,
    inter_source,
    inter_kind,
    inter_count,
    *,
    interpret=False,
):
    def call(*args, limit=VMEM_LIMIT, **kw):
        params = pltpu.CompilerParams(vmem_limit_bytes=limit)
        return pl.pallas_call(*args, interpret=interpret, compiler_params=params, **kw)

    shape = jax.ShapeDtypeStruct
    dma = pltpu.SemaphoreType.DMA
    branch, fine = child_phase.shape
    columns = child_field.shape[2]
    waves = columns // branch
    fine_t, coarse_t = theta_interp.shape
    fine_p, coarse_p = phi_interp.shape
    groups = coarse_p // SUB
    narrow = BLOCK // fine_p * coarse_p
    members = lax.axis_size("mem")
    grp_count = lax.axis_size("grp")
    per_member = fine // members
    targets, slots = inter_source.shape
    theta_t = theta_interp.T
    phi_t = phi_interp.T
    factors = jnp.transpose(translation, (1, 0, 2))
    block = (members, 2, waves, per_member)
    field = child_field.reshape(2, coarse_t, groups, SUB, columns)
    mid = pltpu.VMEM((fine_t, groups, SUB, 2 * columns), f32)
    phases = (branch, fine)

    summed = call(
        aggregate_kernel,
        out_shape=shape(block, f32),
        in_specs=[hbm()] * 4,
        out_specs=vmem(),
        scratch_shapes=[
            pltpu.VMEM(field.shape, f32),
            pltpu.VMEM(theta_t.shape, f32),
            pltpu.VMEM(phi_t.shape, f32),
            pltpu.VMEM(phases, f32),
            mid,
            pltpu.VMEM(phases, f32),
            pltpu.VMEM(phases, f32),
            dma((groups,)),
            dma((3,)),
        ],
        name="aggregate",

    )(*[pltpu.with_memory_space_constraint(v, pltpu.HBM) for v in (field, theta_t, phi_t, child_phase)])

    def exchange(x):
        return lax.all_to_all(x, "mem", split_axis=0, concat_axis=0, tiled=True)

    def swap(x, first):
        pairs = [(i, i + 1) for i in range(first, grp_count - 1, 2)]
        return lax.ppermute(x, "grp", pairs + [(j, i) for i, j in pairs])

    own = exchange(summed)
    far = swap(own, 1)
    twin = swap(own, 0)
    group = lax.axis_index("grp").astype(jnp.int32).reshape(1)
    near_cost = pl.CostEstimate(flops=COST, transcendentals=0, bytes_accessed=1 << 20)
    partial, far_list, far_count, theta_w, phi_w, cosine, sine = call(
        near_kernel,
        out_shape=(
            shape(block, f32),
            shape((targets, slots + 1), jnp.int32),
            shape((targets,), jnp.int32),
            shape((coarse_t * SUB, 3 * fine_t * SUB), bf16),
            shape((BLOCK, 2 * narrow), bf16),
            shape(phases, f32),
            shape(phases, f32),
        ),
        in_specs=[smem()] * 4 + [vmem()] * 6,
        out_specs=(vmem(), smem(), smem(), vmem(), vmem(), vmem(), vmem()),
        scratch_shapes=[
            pltpu.SMEM((targets, slots + 1), jnp.int32),
            pltpu.SMEM((targets,), jnp.int32),
            pltpu.VMEM((2 * members,) + block[1:], f32),
        ],
        name="near",
        cost_estimate=near_cost,
    )(inter_source, inter_kind, inter_count, group, factors, own, twin, theta_t, phi_t, child_phase)

    incoming = call(
        far_kernel,
        out_shape=shape(block, f32),
        in_specs=[smem()] * 2 + [vmem()] * 3,
        out_specs=vmem(),
        name="far",
    )(far_list, far_count, factors, far, partial)

    out = call(
        disaggregate_kernel,
        out_shape=shape(field.shape, f32),
        in_specs=[vmem()] * 5,
        out_specs=hbm(),
        scratch_shapes=[pltpu.VMEM(field.shape, f32), mid, dma((groups,))],
        name="disaggregate",
    )(exchange(incoming), theta_w, phi_w, cosine, sine)
    return out.reshape(child_field.shape)


def solution(mesh):
    return jax.shard_map(
        per_device,
        mesh=mesh,
        in_specs=(
            P(None, None, ("grp", "mem")),
            P(),
            P(),
            P(),
            P(None, None, "mem"),
            P("grp", None),
            P("grp", None),
            P("grp"),
        ),
        out_specs=P(None, None, ("grp", "mem")),
        check_vma=False,
    )
```

```python
import jax
import jax.numpy as jnp
from jax import lax
from jax.experimental import pallas as pl
from jax.experimental.pallas import tpu as pltpu
from jax.sharding import PartitionSpec as P

f32 = jnp.float32
bf16 = jnp.bfloat16
SUB = 8
BLOCK = 256
UNROLL = 4
PAIR = 16
COST = 50_000_000
VMEM_LIMIT = 20 << 20
VMEM_WHOLE = 60 * 1024 * 1024


def split(x):
    hi = x.astype(bf16)
    lo = (x - hi.astype(f32)).astype(bf16)
    return hi, lo


def seat(member, members):
    half = member // 2
    return half + (member % 2) * (members - 1 - 2 * half)


def seating(members):
    return sorted(range(members), key=lambda m: seat(m, members))


def mm(a, b):
    return jnp.dot(a, b, preferred_element_type=f32)


def mm_tn(a, b):
    return lax.dot_general(a, b, (((0,), (0,)), ((), ())), preferred_element_type=f32)


def iota(shape, dim):
    return lax.broadcasted_iota(jnp.int32, shape, dim)


def picker(shape, test):
    return jnp.where(test(iota(shape, 0), iota(shape, 1)), 1.0, 0.0).astype(bf16)


def sincos(q):
    r = q * 0.5
    z = r * r
    s = 1.0 / 6227020800.0
    for c in (-1.0 / 39916800.0, 1.0 / 362880.0, -1.0 / 5040.0, 1.0 / 120.0, -1.0 / 6.0, 1.0):
        s = s * z + c
    s = s * r
    k = 1.0 / 479001600.0
    for c in (-1.0 / 3628800.0, 1.0 / 40320.0, -1.0 / 720.0, 1.0 / 24.0, -0.5, 1.0):
        k = k * z + c
    return 2.0 * s * k, 1.0 - 2.0 * s * s


def theta_rows(part, count, spread, keep):
    rows = spread(part)
    wide = rows.shape[1]
    rows = jnp.broadcast_to(rows[:, None, :], (count, SUB, wide)).reshape(count * SUB, wide)
    return jnp.where(keep, rows, 0.0).astype(bf16)


def aggregate_kernel(x_ref, theta_ref, phi_ref, phase_ref, o_ref, cos_ref, sin_ref, x_buf, theta_buf, phi_buf, phase_buf, mid_ref, x_sems, sems):
    coarse_t, fine_t = theta_ref.shape
    coarse_p, fine_p = phi_ref.shape
    groups = coarse_p // SUB
    span = BLOCK // fine_p
    members, _, waves, per_member = o_ref.shape
    branch, fine = phase_ref.shape
    columns = branch * waves

    small = [
        pltpu.make_async_copy(a, b, sems.at[i])
        for i, (a, b) in enumerate(((theta_ref, theta_buf), (phi_ref, phi_buf), (phase_ref, phase_buf)))
    ]
    large = [pltpu.make_async_copy(x_ref.at[:, :, g], x_buf.at[:, :, g], x_sems.at[g]) for g in range(groups)]
    for copy in small + large:
        copy.start()
    for copy in small:
        copy.wait()

    spread_t = picker((coarse_t, coarse_t * SUB), lambda r, c: r == c // SUB)
    big = (fine_t * SUB, coarse_t * SUB)
    keep = iota(big, 0) % SUB == iota(big, 1) % SUB
    kh, kl = [theta_rows(part, fine_t, lambda p: mm_tn(p, spread_t), keep) for part in split(theta_buf[...])]
    weights = jnp.concatenate([kh, kh, kl], axis=1)

    spread_p = picker((fine_p, BLOCK), lambda r, c: r == c % fine_p)
    shape = (span * coarse_p, BLOCK)
    diag = iota(shape, 0) // coarse_p == iota(shape, 1) // fine_p

    def phi_block(part):
        rows = jnp.concatenate([mm(part, spread_p)] * span, axis=0)
        return jnp.where(diag, rows, 0.0).astype(bf16)

    bh, bl = [phi_block(part) for part in split(phi_buf[...])]
    phi_weights = jnp.concatenate([bh, bh, bl], axis=0)

    sine, cosine = sincos(phase_buf[...])
    cos_ref[...] = cosine
    sin_ref[...] = sine

    for g in range(groups):
        large[g].wait()
        parts = [x_buf[c, :, g].reshape(coarse_t * SUB, columns) for c in range(2)]
        hi, lo = split(jnp.concatenate(parts, axis=1))
        middle = mm(weights, jnp.concatenate([hi, lo, hi], axis=0))
        mid_ref[:, g] = middle.reshape(fine_t, SUB, 2 * columns)

    unit = min(BLOCK, per_member)
    batch = max(per_member, PAIR * BLOCK)
    many = batch // per_member

    def body(step, carry):
        for i in range(batch // BLOCK):
            rows = mid_ref[pl.ds((step * (batch // BLOCK) + i) * span, span)].reshape(span * coarse_p, 2 * columns)
            hi, lo = split(rows.T)
            fine_part = mm(jnp.concatenate([hi, lo, hi], axis=1), phi_weights)
            real = fine_part[:columns].reshape(branch, waves, BLOCK)
            imag = fine_part[columns:].reshape(branch, waves, BLOCK)
            lanes = pl.ds(pl.multiple_of(step * batch + i * BLOCK, BLOCK), BLOCK)
            c = cos_ref[:, lanes][:, None, :]
            s = sin_ref[:, lanes][:, None, :]
            outs = jnp.sum(real * c - imag * s, axis=0), jnp.sum(imag * c + real * s, axis=0)
            for piece in range(BLOCK // unit):
                at = i * BLOCK + piece * unit
                member = seat(step * many + at // per_member, members)
                there = pl.ds(at % per_member, unit)
                for part in range(2):
                    o_ref[member, part, :, there] = outs[part][:, piece * unit : (piece + 1) * unit]
        return carry

    lax.fori_loop(0, fine // batch, body, 0)


def add_slots(entry_of, count, factor_ref, data_ref, acc, wide):
    def slot_body(step, acc):
        real, imag = acc
        for i in range(UNROLL):
            k = step * UNROLL + i
            live = k < count
            entry = jnp.where(live, entry_of(k), 0)
            kind = lax.div(entry, wide)
            at = entry - kind * wide
            factor = factor_ref[kind] * jnp.where(live, 1.0, 0.0).astype(f32)
            fr = factor[0:1]
            fi = factor[1:2]
            sr = data_ref[at, 0]
            si = data_ref[at, 1]
            real = real + (fr * sr - fi * si)
            imag = imag + (fr * si + fi * sr)
        return real, imag

    return lax.fori_loop(0, lax.div(count + (UNROLL - 1), UNROLL), slot_body, acc)


def near_kernel(source_ref, kind_ref, count_ref, group_ref, factor_ref, own_ref, twin_ref, theta_ref, phi_ref, o_ref, far_ref, far_count_ref, theta_out, phi_out, list_ref, near_count_ref, all_ref):
    members = own_ref.shape[0]
    targets, slots = source_ref.shape
    waves, directions = o_ref.shape[2:]
    wide = 2 * members
    group = group_ref[0]
    far_group = group + 2 * (group & 1) - 1

    def sort_target(t, carry):
        count = count_ref[t]

        def sort_slot(k, counts):
            near, far = counts
            source = source_ref[t, k]
            place = lax.div(source, members)
            at = source - place * members
            entry = kind_ref[t, k] * wide + at
            list_ref[t, near] = entry + jnp.where(place == group, 0, members)
            far_ref[t, far] = entry
            is_far = jnp.where(place == far_group, 1, 0)
            return near + 1 - is_far, far + is_far

        near, far = lax.fori_loop(0, count, sort_slot, (0, 0))
        near_count_ref[t] = near
        far_count_ref[t] = far
        return carry

    lax.fori_loop(0, targets, sort_target, 0)

    for m in range(members):
        all_ref[m] = own_ref[seat(m, members)]
        all_ref[members + m] = twin_ref[seat(m, members)]

    def target_body(t, carry):
        zero = jnp.zeros((waves, directions), f32)
        real, imag = add_slots(lambda k: list_ref[t, k], near_count_ref[t], factor_ref, all_ref, (zero, zero), wide)
        o_ref[t, 0] = real
        o_ref[t, 1] = imag
        return carry

    lax.fori_loop(0, targets, target_body, 0)

    coarse_t, fine_t = theta_ref.shape
    coarse_p, fine_p = phi_ref.shape
    span = BLOCK // fine_p
    spread_t = picker((fine_t, fine_t * SUB), lambda r, c: r == c // SUB)
    big = (coarse_t * SUB, fine_t * SUB)
    keep = iota(big, 0) % SUB == iota(big, 1) % SUB
    kh, kl = [theta_rows(part, coarse_t, lambda p: mm(p, spread_t), keep) for part in split(theta_ref[...])]
    theta_out[...] = jnp.concatenate([kh, kh, kl], axis=1)
    narrow = span * coarse_p
    spread_p = picker((coarse_p, narrow), lambda r, c: r == c % coarse_p)
    shape = (BLOCK, narrow)
    diag = iota(shape, 0) // fine_p == iota(shape, 1) // coarse_p

    def phi_block(part):
        rows = jnp.concatenate([mm_tn(part, spread_p)] * span, axis=0)
        return jnp.where(diag, rows, 0.0).astype(bf16)

    phi_out[...] = jnp.concatenate([phi_block(part) for part in split(phi_ref[...])], axis=1)


def far_kernel(far_ref, far_count_ref, factor_ref, far_data_ref, near_ref, o_ref, data_ref):
    targets = near_ref.shape[0]
    members = data_ref.shape[0]
    wide = 2 * members
    for m in range(members):
        data_ref[m] = far_data_ref[seat(m, members)]

    def target_body(t, carry):
        acc = near_ref[t, 0], near_ref[t, 1]
        real, imag = add_slots(lambda k: far_ref[t, k], far_count_ref[t], factor_ref, data_ref, acc, wide)
        o_ref[seat(t, targets), 0] = real
        o_ref[seat(t, targets), 1] = imag
        return carry

    lax.fori_loop(0, targets, target_body, 0)


def disaggregate_kernel(r_ref, weights_ref, phi_weights_ref, cos_ref, sin_ref, o_ref, o_buf, mid_ref, sems):
    fine_t, groups, _, rows = mid_ref.shape
    narrow = phi_weights_ref.shape[1] // 2
    span = narrow // (groups * SUB)
    per_member = r_ref.shape[3]
    columns = rows // 2
    coarse_t = o_ref.shape[1]
    unit = min(BLOCK, per_member)
    many = BLOCK // unit

    def body(pair, carry):
        for i in range(PAIR):
            step = pair * PAIR + i
            parts = [[], []]
            for piece in range(many):
                at = step * BLOCK + piece * unit
                member = lax.div(at, per_member)
                offset = pl.multiple_of(at - member * per_member, unit)
                member = seat(member, r_ref.shape[0])
                for part in range(2):
                    parts[part].append(r_ref[member, part, :, pl.ds(offset, unit)])
            real, imag = [jnp.concatenate(p, axis=1)[None] for p in parts]
            lanes = pl.ds(pl.multiple_of(step * BLOCK, BLOCK), BLOCK)
            c = cos_ref[:, lanes][:, None, :]
            s = sin_ref[:, lanes][:, None, :]
            local = jnp.concatenate(
                [
                    (real * c + imag * s).reshape(columns, BLOCK),
                    (imag * c - real * s).reshape(columns, BLOCK),
                ],
                axis=0,
            )
            hi, lo = split(local)
            y = mm(jnp.concatenate([hi, lo], axis=0), phi_weights_ref[...])
            folded = y[:rows, :narrow] + (y[rows:, :narrow] + y[:rows, narrow:])
            mid_ref[pl.ds(step * span, span)] = folded.T.reshape(span, groups, SUB, rows)
        return carry

    lax.fori_loop(0, fine_t // span // PAIR, body, 0)

    copies = []
    for g in range(groups):
        hi, lo = split(mid_ref[:, g].reshape(fine_t * SUB, rows))
        coarse = mm(weights_ref[...], jnp.concatenate([hi, lo, hi], axis=0))
        for part in range(2):
            o_buf[part, :, g] = coarse[:, part * columns : (part + 1) * columns].reshape(coarse_t, SUB, columns)
        copies.append(pltpu.make_async_copy(o_buf.at[:, :, g], o_ref.at[:, :, g], sems.at[g]))
        copies[-1].start()
    for copy in copies:
        copy.wait()


def vmem():
    return pl.BlockSpec(memory_space=pltpu.VMEM)


def smem():
    return pl.BlockSpec(memory_space=pltpu.SMEM)


def hbm():
    return pl.BlockSpec(memory_space=pltpu.HBM)


def per_device(
    child_field,
    theta_interp,
    phi_interp,
    child_phase,
    translation,
    inter_source,
    inter_kind,
    inter_count,
    *,
    interpret=False,
):
    def call(*args, limit=VMEM_LIMIT, **kw):
        params = pltpu.CompilerParams(vmem_limit_bytes=limit)
        return pl.pallas_call(*args, interpret=interpret, compiler_params=params, **kw)

    shape = jax.ShapeDtypeStruct
    dma = pltpu.SemaphoreType.DMA
    branch, fine = child_phase.shape
    columns = child_field.shape[2]
    waves = columns // branch
    fine_t, coarse_t = theta_interp.shape
    fine_p, coarse_p = phi_interp.shape
    groups = coarse_p // SUB
    narrow = BLOCK // fine_p * coarse_p
    members = lax.axis_size("mem")
    grp_count = lax.axis_size("grp")
    per_member = fine // members
    targets, slots = inter_source.shape
    theta_t = theta_interp.T
    phi_t = phi_interp.T
    factors = jnp.transpose(translation, (1, 0, 2))
    block = (members, 2, waves, per_member)
    field = child_field.reshape(2, coarse_t, groups, SUB, columns)
    mid = pltpu.VMEM((fine_t, groups, SUB, 2 * columns), f32)
    phases = (branch, fine)

    summed, cosine, sine = call(
        aggregate_kernel,
        out_shape=(shape(block, f32), shape(phases, f32), shape(phases, f32)),
        in_specs=[hbm()] * 4,
        out_specs=(vmem(), vmem(), vmem()),
        scratch_shapes=[
            pltpu.VMEM(field.shape, f32),
            pltpu.VMEM(theta_t.shape, f32),
            pltpu.VMEM(phi_t.shape, f32),
            pltpu.VMEM(phases, f32),
            mid,
            dma((groups,)),
            dma((3,)),
        ],
        name="aggregate",

    )(*[pltpu.with_memory_space_constraint(v, pltpu.HBM) for v in (field, theta_t, phi_t, child_phase)])

    def exchange(x):
        return lax.all_to_all(x, "mem", split_axis=0, concat_axis=0, tiled=True, axis_index_groups=[seating(members)])

    def swap(x, first):
        pairs = [(i, i + 1) for i in range(first, grp_count - 1, 2)]
        return lax.ppermute(x, "grp", pairs + [(j, i) for i, j in pairs])

    own = exchange(summed)
    far = swap(own, 1)
    twin = swap(own, 0)
    group = lax.axis_index("grp").astype(jnp.int32).reshape(1)
    near_cost = pl.CostEstimate(flops=COST, transcendentals=0, bytes_accessed=1 << 20)
    partial, far_list, far_count, theta_w, phi_w = call(
        near_kernel,
        out_shape=(
            shape(block, f32),
            shape((targets, slots + 1), jnp.int32),
            shape((targets,), jnp.int32),
            shape((coarse_t * SUB, 3 * fine_t * SUB), bf16),
            shape((BLOCK, 2 * narrow), bf16),
        ),
        in_specs=[smem()] * 4 + [vmem()] * 5,
        out_specs=(vmem(), smem(), smem(), vmem(), vmem()),
        scratch_shapes=[
            pltpu.SMEM((targets, slots + 1), jnp.int32),
            pltpu.SMEM((targets,), jnp.int32),
            pltpu.VMEM((2 * members,) + block[1:], f32),
        ],
        name="near",
        cost_estimate=near_cost,
    )(inter_source, inter_kind, inter_count, group, factors, own, twin, theta_t, phi_t)

    incoming = call(
        far_kernel,
        out_shape=shape(block, f32),
        in_specs=[smem()] * 2 + [vmem()] * 3,
        out_specs=vmem(),
        scratch_shapes=[pltpu.VMEM(block, f32)],
        name="far",
    )(far_list, far_count, factors, far, partial)

    out = call(
        disaggregate_kernel,
        out_shape=shape(field.shape, f32),
        in_specs=[vmem()] * 5,
        out_specs=hbm(),
        scratch_shapes=[pltpu.VMEM(field.shape, f32), mid, dma((groups,))],
        name="disaggregate",
    )(exchange(incoming), theta_w, phi_w, cosine, sine)
    return out.reshape(child_field.shape)


def solution(mesh):
    return jax.shard_map(
        per_device,
        mesh=mesh,
        in_specs=(
            P(None, None, ("grp", "mem")),
            P(),
            P(),
            P(),
            P(None, None, "mem"),
            P("grp", None),
            P("grp", None),
            P("grp"),
        ),
        out_specs=P(None, None, ("grp", "mem")),
        check_vma=False,
    )
```

```python
import jax
import jax.numpy as jnp
from jax import lax
from jax.experimental import pallas as pl
from jax.experimental.pallas import tpu as pltpu
from jax.sharding import PartitionSpec as P

f32 = jnp.float32
bf16 = jnp.bfloat16
SUB = 8
BLOCK = 256
UNROLL = 8
PAIR = 16
COST = 50_000_000
VMEM_LIMIT = 20 << 20
VMEM_WHOLE = 60 * 1024 * 1024


def split(x):
    hi = x.astype(bf16)
    lo = (x - hi.astype(f32)).astype(bf16)
    return hi, lo


def seat(member, members):
    half = member // 2
    return half + (member % 2) * (members - 1 - 2 * half)


def seating(members):
    return sorted(range(members), key=lambda m: seat(m, members))


def mm(a, b):
    return jnp.dot(a, b, preferred_element_type=f32)


def mm_tn(a, b):
    return lax.dot_general(a, b, (((0,), (0,)), ((), ())), preferred_element_type=f32)


def iota(shape, dim):
    return lax.broadcasted_iota(jnp.int32, shape, dim)


def picker(shape, test):
    return jnp.where(test(iota(shape, 0), iota(shape, 1)), 1.0, 0.0).astype(bf16)


def sincos(q):
    r = q * 0.5
    z = r * r
    s = 1.0 / 6227020800.0
    for c in (-1.0 / 39916800.0, 1.0 / 362880.0, -1.0 / 5040.0, 1.0 / 120.0, -1.0 / 6.0, 1.0):
        s = s * z + c
    s = s * r
    k = 1.0 / 479001600.0
    for c in (-1.0 / 3628800.0, 1.0 / 40320.0, -1.0 / 720.0, 1.0 / 24.0, -0.5, 1.0):
        k = k * z + c
    return 2.0 * s * k, 1.0 - 2.0 * s * s


def theta_rows(part, count, spread, keep):
    rows = spread(part)
    wide = rows.shape[1]
    rows = jnp.broadcast_to(rows[:, None, :], (count, SUB, wide)).reshape(count * SUB, wide)
    return jnp.where(keep, rows, 0.0).astype(bf16)


def aggregate_kernel(x_ref, theta_ref, phi_ref, phase_ref, o_ref, cos_ref, sin_ref, x_buf, theta_buf, phi_buf, phase_buf, mid_ref, x_sems, sems):
    coarse_t, fine_t = theta_ref.shape
    coarse_p, fine_p = phi_ref.shape
    groups = coarse_p // SUB
    span = BLOCK // fine_p
    members, _, waves, per_member = o_ref.shape
    branch, fine = phase_ref.shape
    columns = branch * waves

    small = [
        pltpu.make_async_copy(a, b, sems.at[i])
        for i, (a, b) in enumerate(((theta_ref, theta_buf), (phi_ref, phi_buf), (phase_ref, phase_buf)))
    ]
    large = [pltpu.make_async_copy(x_ref.at[:, :, g], x_buf.at[:, :, g], x_sems.at[g]) for g in range(groups)]
    for copy in small + large:
        copy.start()
    for copy in small:
        copy.wait()

    spread_t = picker((coarse_t, coarse_t * SUB), lambda r, c: r == c // SUB)
    big = (fine_t * SUB, coarse_t * SUB)
    keep = iota(big, 0) % SUB == iota(big, 1) % SUB
    kh, kl = [theta_rows(part, fine_t, lambda p: mm_tn(p, spread_t), keep) for part in split(theta_buf[...])]
    weights = jnp.concatenate([kh, kh, kl], axis=1)

    spread_p = picker((fine_p, BLOCK), lambda r, c: r == c % fine_p)
    shape = (span * coarse_p, BLOCK)
    diag = iota(shape, 0) // coarse_p == iota(shape, 1) // fine_p

    def phi_block(part):
        rows = jnp.concatenate([mm(part, spread_p)] * span, axis=0)
        return jnp.where(diag, rows, 0.0).astype(bf16)

    bh, bl = [phi_block(part) for part in split(phi_buf[...])]
    phi_weights = jnp.concatenate([bh, bh, bl], axis=0)

    sine, cosine = sincos(phase_buf[...])
    cos_ref[...] = cosine
    sin_ref[...] = sine

    for g in range(groups):
        large[g].wait()
        parts = [x_buf[c, :, g].reshape(coarse_t * SUB, columns) for c in range(2)]
        hi, lo = split(jnp.concatenate(parts, axis=1))
        middle = mm(weights, jnp.concatenate([hi, lo, hi], axis=0))
        mid_ref[:, g] = middle.reshape(fine_t, SUB, 2 * columns)

    unit = min(BLOCK, per_member)
    batch = max(per_member, PAIR * BLOCK)
    many = batch // per_member

    def body(step, carry):
        for i in range(batch // BLOCK):
            rows = mid_ref[pl.ds((step * (batch // BLOCK) + i) * span, span)].reshape(span * coarse_p, 2 * columns)
            hi, lo = split(rows.T)
            fine_part = mm(jnp.concatenate([hi, lo, hi], axis=1), phi_weights)
            real = fine_part[:columns].reshape(branch, waves, BLOCK)
            imag = fine_part[columns:].reshape(branch, waves, BLOCK)
            lanes = pl.ds(pl.multiple_of(step * batch + i * BLOCK, BLOCK), BLOCK)
            c = cos_ref[:, lanes][:, None, :]
            s = sin_ref[:, lanes][:, None, :]
            outs = jnp.sum(real * c - imag * s, axis=0), jnp.sum(imag * c + real * s, axis=0)
            for piece in range(BLOCK // unit):
                at = i * BLOCK + piece * unit
                member = seat(step * many + at // per_member, members)
                there = pl.ds(at % per_member, unit)
                for part in range(2):
                    o_ref[member, part, :, there] = outs[part][:, piece * unit : (piece + 1) * unit]
        return carry

    lax.fori_loop(0, fine // batch, body, 0)


def add_slots(entry_of, count, factor_ref, data_ref, acc, wide):
    def slot_body(step, acc):
        real, imag = acc
        for i in range(UNROLL):
            k = step * UNROLL + i
            live = k < count
            entry = jnp.where(live, entry_of(k), 0)
            kind = lax.div(entry, wide)
            at = entry - kind * wide
            factor = factor_ref[kind] * jnp.where(live, 1.0, 0.0).astype(f32)
            fr = factor[0:1]
            fi = factor[1:2]
            sr = data_ref[at, 0]
            si = data_ref[at, 1]
            real = real + (fr * sr - fi * si)
            imag = imag + (fr * si + fi * sr)
        return real, imag

    return lax.fori_loop(0, lax.div(count + (UNROLL - 1), UNROLL), slot_body, acc)


def near_kernel(source_ref, kind_ref, count_ref, group_ref, factor_ref, own_ref, twin_ref, theta_ref, phi_ref, o_ref, far_ref, far_count_ref, theta_out, phi_out, list_ref, near_count_ref, all_ref):
    members = own_ref.shape[0]
    targets, slots = source_ref.shape
    waves, directions = o_ref.shape[2:]
    wide = 2 * members
    group = group_ref[0]
    far_group = group + 2 * (group & 1) - 1

    def sort_target(t, carry):
        count = count_ref[t]

        def sort_slot(k, counts):
            near, far = counts
            source = source_ref[t, k]
            place = lax.div(source, members)
            at = source - place * members
            entry = kind_ref[t, k] * wide + at
            list_ref[t, near] = entry + jnp.where(place == group, 0, members)
            far_ref[t, far] = entry
            is_far = jnp.where(place == far_group, 1, 0)
            return near + 1 - is_far, far + is_far

        near, far = lax.fori_loop(0, count, sort_slot, (0, 0))
        near_count_ref[t] = near
        far_count_ref[t] = far
        return carry

    lax.fori_loop(0, targets, sort_target, 0)

    for m in range(members):
        all_ref[m] = own_ref[seat(m, members)]
        all_ref[members + m] = twin_ref[seat(m, members)]

    def target_body(t, carry):
        zero = jnp.zeros((waves, directions), f32)
        real, imag = add_slots(lambda k: list_ref[t, k], near_count_ref[t], factor_ref, all_ref, (zero, zero), wide)
        o_ref[t, 0] = real
        o_ref[t, 1] = imag
        return carry

    lax.fori_loop(0, targets, target_body, 0)

    coarse_t, fine_t = theta_ref.shape
    coarse_p, fine_p = phi_ref.shape
    span = BLOCK // fine_p
    spread_t = picker((fine_t, fine_t * SUB), lambda r, c: r == c // SUB)
    big = (coarse_t * SUB, fine_t * SUB)
    keep = iota(big, 0) % SUB == iota(big, 1) % SUB
    kh, kl = [theta_rows(part, coarse_t, lambda p: mm(p, spread_t), keep) for part in split(theta_ref[...])]
    theta_out[...] = jnp.concatenate([kh, kh, kl], axis=1)
    narrow = span * coarse_p
    spread_p = picker((coarse_p, narrow), lambda r, c: r == c % coarse_p)
    shape = (BLOCK, narrow)
    diag = iota(shape, 0) // fine_p == iota(shape, 1) // coarse_p

    def phi_block(part):
        rows = jnp.concatenate([mm_tn(part, spread_p)] * span, axis=0)
        return jnp.where(diag, rows, 0.0).astype(bf16)

    phi_out[...] = jnp.concatenate([phi_block(part) for part in split(phi_ref[...])], axis=1)


def far_kernel(far_ref, far_count_ref, factor_ref, far_data_ref, near_ref, o_ref, data_ref):
    targets = near_ref.shape[0]
    members = data_ref.shape[0]
    wide = 2 * members
    for m in range(members):
        data_ref[m] = far_data_ref[seat(m, members)]

    def target_body(t, carry):
        acc = near_ref[t, 0], near_ref[t, 1]
        real, imag = add_slots(lambda k: far_ref[t, k], far_count_ref[t], factor_ref, data_ref, acc, wide)
        o_ref[seat(t, targets), 0] = real
        o_ref[seat(t, targets), 1] = imag
        return carry

    lax.fori_loop(0, targets, target_body, 0)


def disaggregate_kernel(r_ref, weights_ref, phi_weights_ref, cos_ref, sin_ref, o_ref, o_buf, mid_ref, sems):
    fine_t, groups, _, rows = mid_ref.shape
    narrow = phi_weights_ref.shape[1] // 2
    span = narrow // (groups * SUB)
    per_member = r_ref.shape[3]
    columns = rows // 2
    coarse_t = o_ref.shape[1]
    unit = min(BLOCK, per_member)
    many = BLOCK // unit

    def body(pair, carry):
        for i in range(PAIR):
            step = pair * PAIR + i
            parts = [[], []]
            for piece in range(many):
                at = step * BLOCK + piece * unit
                member = lax.div(at, per_member)
                offset = pl.multiple_of(at - member * per_member, unit)
                member = seat(member, r_ref.shape[0])
                for part in range(2):
                    parts[part].append(r_ref[member, part, :, pl.ds(offset, unit)])
            real, imag = [jnp.concatenate(p, axis=1)[None] for p in parts]
            lanes = pl.ds(pl.multiple_of(step * BLOCK, BLOCK), BLOCK)
            c = cos_ref[:, lanes][:, None, :]
            s = sin_ref[:, lanes][:, None, :]
            local = jnp.concatenate(
                [
                    (real * c + imag * s).reshape(columns, BLOCK),
                    (imag * c - real * s).reshape(columns, BLOCK),
                ],
                axis=0,
            )
            hi, lo = split(local)
            y = mm(jnp.concatenate([hi, lo], axis=0), phi_weights_ref[...])
            folded = y[:rows, :narrow] + (y[rows:, :narrow] + y[:rows, narrow:])
            mid_ref[pl.ds(step * span, span)] = folded.T.reshape(span, groups, SUB, rows)
        return carry

    lax.fori_loop(0, fine_t // span // PAIR, body, 0)

    copies = []
    for g in range(groups):
        hi, lo = split(mid_ref[:, g].reshape(fine_t * SUB, rows))
        coarse = mm(weights_ref[...], jnp.concatenate([hi, lo, hi], axis=0))
        for part in range(2):
            o_buf[part, :, g] = coarse[:, part * columns : (part + 1) * columns].reshape(coarse_t, SUB, columns)
        copies.append(pltpu.make_async_copy(o_buf.at[:, :, g], o_ref.at[:, :, g], sems.at[g]))
        copies[-1].start()
    for copy in copies:
        copy.wait()


def vmem():
    return pl.BlockSpec(memory_space=pltpu.VMEM)


def smem():
    return pl.BlockSpec(memory_space=pltpu.SMEM)


def hbm():
    return pl.BlockSpec(memory_space=pltpu.HBM)


def per_device(
    child_field,
    theta_interp,
    phi_interp,
    child_phase,
    translation,
    inter_source,
    inter_kind,
    inter_count,
    *,
    interpret=False,
):
    def call(*args, limit=VMEM_LIMIT, **kw):
        params = pltpu.CompilerParams(vmem_limit_bytes=limit)
        return pl.pallas_call(*args, interpret=interpret, compiler_params=params, **kw)

    shape = jax.ShapeDtypeStruct
    dma = pltpu.SemaphoreType.DMA
    branch, fine = child_phase.shape
    columns = child_field.shape[2]
    waves = columns // branch
    fine_t, coarse_t = theta_interp.shape
    fine_p, coarse_p = phi_interp.shape
    groups = coarse_p // SUB
    narrow = BLOCK // fine_p * coarse_p
    members = lax.axis_size("mem")
    grp_count = lax.axis_size("grp")
    per_member = fine // members
    targets, slots = inter_source.shape
    theta_t = theta_interp.T
    phi_t = phi_interp.T
    factors = jnp.transpose(translation, (1, 0, 2))
    block = (members, 2, waves, per_member)
    field = child_field.reshape(2, coarse_t, groups, SUB, columns)
    mid = pltpu.VMEM((fine_t, groups, SUB, 2 * columns), f32)
    phases = (branch, fine)

    summed, cosine, sine = call(
        aggregate_kernel,
        out_shape=(shape(block, f32), shape(phases, f32), shape(phases, f32)),
        in_specs=[hbm()] * 4,
        out_specs=(vmem(), vmem(), vmem()),
        scratch_shapes=[
            pltpu.VMEM(field.shape, f32),
            pltpu.VMEM(theta_t.shape, f32),
            pltpu.VMEM(phi_t.shape, f32),
            pltpu.VMEM(phases, f32),
            mid,
            dma((groups,)),
            dma((3,)),
        ],
        name="aggregate",

    )(*[pltpu.with_memory_space_constraint(v, pltpu.HBM) for v in (field, theta_t, phi_t, child_phase)])

    def exchange(x):
        return lax.all_to_all(x, "mem", split_axis=0, concat_axis=0, tiled=True, axis_index_groups=[seating(members)])

    def swap(x, first):
        pairs = [(i, i + 1) for i in range(first, grp_count - 1, 2)]
        return lax.ppermute(x, "grp", pairs + [(j, i) for i, j in pairs])

    own = exchange(summed)
    far = swap(own, 1)
    twin = swap(own, 0)
    group = lax.axis_index("grp").astype(jnp.int32).reshape(1)
    near_cost = pl.CostEstimate(flops=COST, transcendentals=0, bytes_accessed=1 << 20)
    partial, far_list, far_count, theta_w, phi_w = call(
        near_kernel,
        out_shape=(
            shape(block, f32),
            shape((targets, slots + 1), jnp.int32),
            shape((targets,), jnp.int32),
            shape((coarse_t * SUB, 3 * fine_t * SUB), bf16),
            shape((BLOCK, 2 * narrow), bf16),
        ),
        in_specs=[smem()] * 4 + [vmem()] * 5,
        out_specs=(vmem(), smem(), smem(), vmem(), vmem()),
        scratch_shapes=[
            pltpu.SMEM((targets, slots + 1), jnp.int32),
            pltpu.SMEM((targets,), jnp.int32),
            pltpu.VMEM((2 * members,) + block[1:], f32),
        ],
        name="near",
        cost_estimate=near_cost,
    )(inter_source, inter_kind, inter_count, group, factors, own, twin, theta_t, phi_t)

    incoming = call(
        far_kernel,
        out_shape=shape(block, f32),
        in_specs=[smem()] * 2 + [vmem()] * 3,
        out_specs=vmem(),
        scratch_shapes=[pltpu.VMEM(block, f32)],
        name="far",
    )(far_list, far_count, factors, far, partial)

    out = call(
        disaggregate_kernel,
        out_shape=shape(field.shape, f32),
        in_specs=[vmem()] * 5,
        out_specs=hbm(),
        scratch_shapes=[pltpu.VMEM(field.shape, f32), mid, dma((groups,))],
        name="disaggregate",
    )(exchange(incoming), theta_w, phi_w, cosine, sine)
    return out.reshape(child_field.shape)


def solution(mesh):
    return jax.shard_map(
        per_device,
        mesh=mesh,
        in_specs=(
            P(None, None, ("grp", "mem")),
            P(),
            P(),
            P(),
            P(None, None, "mem"),
            P("grp", None),
            P("grp", None),
            P("grp"),
        ),
        out_specs=P(None, None, ("grp", "mem")),
        check_vma=False,
    )
```

```python
import jax
import jax.numpy as jnp
from jax import lax
from jax.experimental import pallas as pl
from jax.experimental.pallas import tpu as pltpu
from jax.sharding import PartitionSpec as P

f32 = jnp.float32
bf16 = jnp.bfloat16
SUB = 8
BLOCK = 256
UNROLL = 8
FAR_UNROLL = 4
PAIR = 16
COST = 50_000_000
VMEM_LIMIT = 20 << 20
VMEM_WHOLE = 60 * 1024 * 1024


def split(x):
    hi = x.astype(bf16)
    lo = (x - hi.astype(f32)).astype(bf16)
    return hi, lo


def seat(member, members):
    half = member // 2
    return half + (member % 2) * (members - 1 - 2 * half)


def seating(members):
    return sorted(range(members), key=lambda m: seat(m, members))


def mm(a, b):
    return jnp.dot(a, b, preferred_element_type=f32)


def mm_tn(a, b):
    return lax.dot_general(a, b, (((0,), (0,)), ((), ())), preferred_element_type=f32)


def iota(shape, dim):
    return lax.broadcasted_iota(jnp.int32, shape, dim)


def picker(shape, test):
    return jnp.where(test(iota(shape, 0), iota(shape, 1)), 1.0, 0.0).astype(bf16)


def sincos(q):
    r = q * 0.5
    z = r * r
    s = 1.0 / 6227020800.0
    for c in (-1.0 / 39916800.0, 1.0 / 362880.0, -1.0 / 5040.0, 1.0 / 120.0, -1.0 / 6.0, 1.0):
        s = s * z + c
    s = s * r
    k = 1.0 / 479001600.0
    for c in (-1.0 / 3628800.0, 1.0 / 40320.0, -1.0 / 720.0, 1.0 / 24.0, -0.5, 1.0):
        k = k * z + c
    return 2.0 * s * k, 1.0 - 2.0 * s * s


def theta_rows(part, count, spread, keep):
    rows = spread(part)
    wide = rows.shape[1]
    rows = jnp.broadcast_to(rows[:, None, :], (count, SUB, wide)).reshape(count * SUB, wide)
    return jnp.where(keep, rows, 0.0).astype(bf16)


def aggregate_kernel(x_ref, theta_ref, phi_ref, phase_ref, o_ref, cos_ref, sin_ref, x_buf, theta_buf, phi_buf, phase_buf, mid_ref, x_sems, sems):
    coarse_t, fine_t = theta_ref.shape
    coarse_p, fine_p = phi_ref.shape
    groups = coarse_p // SUB
    span = BLOCK // fine_p
    members, _, waves, per_member = o_ref.shape
    branch, fine = phase_ref.shape
    columns = branch * waves

    small = [
        pltpu.make_async_copy(a, b, sems.at[i])
        for i, (a, b) in enumerate(((theta_ref, theta_buf), (phi_ref, phi_buf), (phase_ref, phase_buf)))
    ]
    large = [pltpu.make_async_copy(x_ref.at[:, :, g], x_buf.at[:, :, g], x_sems.at[g]) for g in range(groups)]
    for copy in small + large:
        copy.start()
    for copy in small:
        copy.wait()

    spread_t = picker((coarse_t, coarse_t * SUB), lambda r, c: r == c // SUB)
    big = (fine_t * SUB, coarse_t * SUB)
    keep = iota(big, 0) % SUB == iota(big, 1) % SUB
    kh, kl = [theta_rows(part, fine_t, lambda p: mm_tn(p, spread_t), keep) for part in split(theta_buf[...])]
    weights = jnp.concatenate([kh, kh, kl], axis=1)

    spread_p = picker((fine_p, BLOCK), lambda r, c: r == c % fine_p)
    shape = (span * coarse_p, BLOCK)
    diag = iota(shape, 0) // coarse_p == iota(shape, 1) // fine_p

    def phi_block(part):
        rows = jnp.concatenate([mm(part, spread_p)] * span, axis=0)
        return jnp.where(diag, rows, 0.0).astype(bf16)

    bh, bl = [phi_block(part) for part in split(phi_buf[...])]
    phi_weights = jnp.concatenate([bh, bh, bl], axis=0)

    sine, cosine = sincos(phase_buf[...])
    cos_ref[...] = cosine
    sin_ref[...] = sine

    for g in range(groups):
        large[g].wait()
        parts = [x_buf[c, :, g].reshape(coarse_t * SUB, columns) for c in range(2)]
        hi, lo = split(jnp.concatenate(parts, axis=1))
        middle = mm(weights, jnp.concatenate([hi, lo, hi], axis=0))
        mid_ref[:, g] = middle.reshape(fine_t, SUB, 2 * columns)

    unit = min(BLOCK, per_member)
    batch = max(per_member, PAIR * BLOCK)
    many = batch // per_member

    def body(step, carry):
        for i in range(batch // BLOCK):
            rows = mid_ref[pl.ds((step * (batch // BLOCK) + i) * span, span)].reshape(span * coarse_p, 2 * columns)
            hi, lo = split(rows.T)
            fine_part = mm(jnp.concatenate([hi, lo, hi], axis=1), phi_weights)
            real = fine_part[:columns].reshape(branch, waves, BLOCK)
            imag = fine_part[columns:].reshape(branch, waves, BLOCK)
            lanes = pl.ds(pl.multiple_of(step * batch + i * BLOCK, BLOCK), BLOCK)
            c = cos_ref[:, lanes][:, None, :]
            s = sin_ref[:, lanes][:, None, :]
            outs = jnp.sum(real * c - imag * s, axis=0), jnp.sum(imag * c + real * s, axis=0)
            for piece in range(BLOCK // unit):
                at = i * BLOCK + piece * unit
                member = seat(step * many + at // per_member, members)
                there = pl.ds(at % per_member, unit)
                for part in range(2):
                    o_ref[member, part, :, there] = outs[part][:, piece * unit : (piece + 1) * unit]
        return carry

    lax.fori_loop(0, fine // batch, body, 0)


def add_slots(entry_of, count, factor_ref, data_ref, acc, wide, unroll):
    def slot_body(step, acc):
        real, imag = acc
        for i in range(unroll):
            k = step * unroll + i
            live = k < count
            entry = jnp.where(live, entry_of(k), 0)
            kind = lax.div(entry, wide)
            at = entry - kind * wide
            factor = factor_ref[kind] * jnp.where(live, 1.0, 0.0).astype(f32)
            fr = factor[0:1]
            fi = factor[1:2]
            sr = data_ref[at, 0]
            si = data_ref[at, 1]
            real = real + (fr * sr - fi * si)
            imag = imag + (fr * si + fi * sr)
        return real, imag

    return lax.fori_loop(0, lax.div(count + (unroll - 1), unroll), slot_body, acc)


def near_kernel(source_ref, kind_ref, count_ref, group_ref, factor_ref, own_ref, twin_ref, theta_ref, phi_ref, o_ref, far_ref, far_count_ref, theta_out, phi_out, list_ref, near_count_ref, all_ref):
    members = own_ref.shape[0]
    targets, slots = source_ref.shape
    waves, directions = o_ref.shape[2:]
    wide = 2 * members
    group = group_ref[0]
    far_group = group + 2 * (group & 1) - 1

    def sort_target(t, carry):
        count = count_ref[t]

        def sort_slot(k, counts):
            near, far = counts
            source = source_ref[t, k]
            place = lax.div(source, members)
            at = source - place * members
            entry = kind_ref[t, k] * wide + at
            list_ref[t, near] = entry + jnp.where(place == group, 0, members)
            far_ref[t, far] = entry
            is_far = jnp.where(place == far_group, 1, 0)
            return near + 1 - is_far, far + is_far

        near, far = lax.fori_loop(0, count, sort_slot, (0, 0))
        near_count_ref[t] = near
        far_count_ref[t] = far
        return carry

    lax.fori_loop(0, targets, sort_target, 0)

    for m in range(members):
        all_ref[m] = own_ref[seat(m, members)]
        all_ref[members + m] = twin_ref[seat(m, members)]

    def target_body(t, carry):
        zero = jnp.zeros((waves, directions), f32)
        real, imag = add_slots(lambda k: list_ref[t, k], near_count_ref[t], factor_ref, all_ref, (zero, zero), wide, UNROLL)
        o_ref[t, 0] = real
        o_ref[t, 1] = imag
        return carry

    lax.fori_loop(0, targets, target_body, 0)

    coarse_t, fine_t = theta_ref.shape
    coarse_p, fine_p = phi_ref.shape
    span = BLOCK // fine_p
    spread_t = picker((fine_t, fine_t * SUB), lambda r, c: r == c // SUB)
    big = (coarse_t * SUB, fine_t * SUB)
    keep = iota(big, 0) % SUB == iota(big, 1) % SUB
    kh, kl = [theta_rows(part, coarse_t, lambda p: mm(p, spread_t), keep) for part in split(theta_ref[...])]
    theta_out[...] = jnp.concatenate([kh, kh, kl], axis=1)
    narrow = span * coarse_p
    spread_p = picker((coarse_p, narrow), lambda r, c: r == c % coarse_p)
    shape = (BLOCK, narrow)
    diag = iota(shape, 0) // fine_p == iota(shape, 1) // coarse_p

    def phi_block(part):
        rows = jnp.concatenate([mm_tn(part, spread_p)] * span, axis=0)
        return jnp.where(diag, rows, 0.0).astype(bf16)

    phi_out[...] = jnp.concatenate([phi_block(part) for part in split(phi_ref[...])], axis=1)


def far_kernel(far_ref, far_count_ref, factor_ref, far_data_ref, near_ref, o_ref, data_ref):
    targets = near_ref.shape[0]
    members = data_ref.shape[0]
    wide = 2 * members
    for m in range(members):
        data_ref[m] = far_data_ref[seat(m, members)]

    def target_body(t, carry):
        acc = near_ref[t, 0], near_ref[t, 1]
        real, imag = add_slots(lambda k: far_ref[t, k], far_count_ref[t], factor_ref, data_ref, acc, wide, FAR_UNROLL)
        o_ref[seat(t, targets), 0] = real
        o_ref[seat(t, targets), 1] = imag
        return carry

    lax.fori_loop(0, targets, target_body, 0)


def disaggregate_kernel(r_ref, weights_ref, phi_weights_ref, cos_ref, sin_ref, o_ref, o_buf, mid_ref, sems):
    fine_t, groups, _, rows = mid_ref.shape
    narrow = phi_weights_ref.shape[1] // 2
    span = narrow // (groups * SUB)
    per_member = r_ref.shape[3]
    columns = rows // 2
    coarse_t = o_ref.shape[1]
    unit = min(BLOCK, per_member)
    many = BLOCK // unit

    def body(pair, carry):
        for i in range(PAIR):
            step = pair * PAIR + i
            parts = [[], []]
            for piece in range(many):
                at = step * BLOCK + piece * unit
                member = lax.div(at, per_member)
                offset = pl.multiple_of(at - member * per_member, unit)
                member = seat(member, r_ref.shape[0])
                for part in range(2):
                    parts[part].append(r_ref[member, part, :, pl.ds(offset, unit)])
            real, imag = [jnp.concatenate(p, axis=1)[None] for p in parts]
            lanes = pl.ds(pl.multiple_of(step * BLOCK, BLOCK), BLOCK)
            c = cos_ref[:, lanes][:, None, :]
            s = sin_ref[:, lanes][:, None, :]
            local = jnp.concatenate(
                [
                    (real * c + imag * s).reshape(columns, BLOCK),
                    (imag * c - real * s).reshape(columns, BLOCK),
                ],
                axis=0,
            )
            hi, lo = split(local)
            y = mm(jnp.concatenate([hi, lo], axis=0), phi_weights_ref[...])
            folded = y[:rows, :narrow] + (y[rows:, :narrow] + y[:rows, narrow:])
            mid_ref[pl.ds(step * span, span)] = folded.T.reshape(span, groups, SUB, rows)
        return carry

    lax.fori_loop(0, fine_t // span // PAIR, body, 0)

    copies = []
    for g in range(groups):
        hi, lo = split(mid_ref[:, g].reshape(fine_t * SUB, rows))
        coarse = mm(weights_ref[...], jnp.concatenate([hi, lo, hi], axis=0))
        for part in range(2):
            o_buf[part, :, g] = coarse[:, part * columns : (part + 1) * columns].reshape(coarse_t, SUB, columns)
        copies.append(pltpu.make_async_copy(o_buf.at[:, :, g], o_ref.at[:, :, g], sems.at[g]))
        copies[-1].start()
    for copy in copies:
        copy.wait()


def vmem():
    return pl.BlockSpec(memory_space=pltpu.VMEM)


def smem():
    return pl.BlockSpec(memory_space=pltpu.SMEM)


def hbm():
    return pl.BlockSpec(memory_space=pltpu.HBM)


def per_device(
    child_field,
    theta_interp,
    phi_interp,
    child_phase,
    translation,
    inter_source,
    inter_kind,
    inter_count,
    *,
    interpret=False,
):
    def call(*args, limit=VMEM_LIMIT, **kw):
        params = pltpu.CompilerParams(vmem_limit_bytes=limit)
        return pl.pallas_call(*args, interpret=interpret, compiler_params=params, **kw)

    shape = jax.ShapeDtypeStruct
    dma = pltpu.SemaphoreType.DMA
    branch, fine = child_phase.shape
    columns = child_field.shape[2]
    waves = columns // branch
    fine_t, coarse_t = theta_interp.shape
    fine_p, coarse_p = phi_interp.shape
    groups = coarse_p // SUB
    narrow = BLOCK // fine_p * coarse_p
    members = lax.axis_size("mem")
    grp_count = lax.axis_size("grp")
    per_member = fine // members
    targets, slots = inter_source.shape
    theta_t = theta_interp.T
    phi_t = phi_interp.T
    factors = jnp.transpose(translation, (1, 0, 2))
    block = (members, 2, waves, per_member)
    field = child_field.reshape(2, coarse_t, groups, SUB, columns)
    mid = pltpu.VMEM((fine_t, groups, SUB, 2 * columns), f32)
    phases = (branch, fine)

    summed, cosine, sine = call(
        aggregate_kernel,
        out_shape=(shape(block, f32), shape(phases, f32), shape(phases, f32)),
        in_specs=[hbm()] * 4,
        out_specs=(vmem(), vmem(), vmem()),
        scratch_shapes=[
            pltpu.VMEM(field.shape, f32),
            pltpu.VMEM(theta_t.shape, f32),
            pltpu.VMEM(phi_t.shape, f32),
            pltpu.VMEM(phases, f32),
            mid,
            dma((groups,)),
            dma((3,)),
        ],
        name="aggregate",

    )(*[pltpu.with_memory_space_constraint(v, pltpu.HBM) for v in (field, theta_t, phi_t, child_phase)])

    def exchange(x):
        return lax.all_to_all(x, "mem", split_axis=0, concat_axis=0, tiled=True, axis_index_groups=[seating(members)])

    def swap(x, first):
        pairs = [(i, i + 1) for i in range(first, grp_count - 1, 2)]
        return lax.ppermute(x, "grp", pairs + [(j, i) for i, j in pairs])

    own = exchange(summed)
    far = swap(own, 1)
    twin = swap(own, 0)
    group = lax.axis_index("grp").astype(jnp.int32).reshape(1)
    near_cost = pl.CostEstimate(flops=COST, transcendentals=0, bytes_accessed=1 << 20)
    partial, far_list, far_count, theta_w, phi_w = call(
        near_kernel,
        out_shape=(
            shape(block, f32),
            shape((targets, slots + 1), jnp.int32),
            shape((targets,), jnp.int32),
            shape((coarse_t * SUB, 3 * fine_t * SUB), bf16),
            shape((BLOCK, 2 * narrow), bf16),
        ),
        in_specs=[smem()] * 4 + [vmem()] * 5,
        out_specs=(vmem(), smem(), smem(), vmem(), vmem()),
        scratch_shapes=[
            pltpu.SMEM((targets, slots + 1), jnp.int32),
            pltpu.SMEM((targets,), jnp.int32),
            pltpu.VMEM((2 * members,) + block[1:], f32),
        ],
        name="near",
        cost_estimate=near_cost,
    )(inter_source, inter_kind, inter_count, group, factors, own, twin, theta_t, phi_t)

    incoming = call(
        far_kernel,
        out_shape=shape(block, f32),
        in_specs=[smem()] * 2 + [vmem()] * 3,
        out_specs=vmem(),
        scratch_shapes=[pltpu.VMEM(block, f32)],
        name="far",
    )(far_list, far_count, factors, far, partial)

    out = call(
        disaggregate_kernel,
        out_shape=shape(field.shape, f32),
        in_specs=[vmem()] * 5,
        out_specs=hbm(),
        scratch_shapes=[pltpu.VMEM(field.shape, f32), mid, dma((groups,))],
        name="disaggregate",
    )(exchange(incoming), theta_w, phi_w, cosine, sine)
    return out.reshape(child_field.shape)


def solution(mesh):
    return jax.shard_map(
        per_device,
        mesh=mesh,
        in_specs=(
            P(None, None, ("grp", "mem")),
            P(),
            P(),
            P(),
            P(None, None, "mem"),
            P("grp", None),
            P("grp", None),
            P("grp"),
        ),
        out_specs=P(None, None, ("grp", "mem")),
        check_vma=False,
    )
```
